128 devices in a mesh: rows: 32 (over z, y, core), vecs: 4 (over x).
Axes of the slice: x: 4, y: 4, z: 4, core: 2. Of those that a mesh axis runs over, the one named last changes fastest.
Arguments:
- basis: bfloat16 [100, 2097152], P('vecs', 'rows'), may hold values from -6 to 6
- coefficients: bfloat16 [100, 40], replicated, may hold values from -0.625 to 0.625
- eigen_values: float32 [40], P('vecs'), may hold values from -3 to 1
- stiffness: float32 [2097152], P('rows'), may hold values from 6.5 to 10
- damping: float32 [2097152], P('rows'), may hold values from 0.2 to 2
- mass: float32 [2097152], P('rows'), may hold values from 0.5 to 2
- link_count: int32 [32], P('rows'), may hold values from 1024 to 4096, as said below
- lower_cells: int32 [32, 4096], P('rows'), may hold values from 0 to 4095
- upper_cells: int32 [32, 4096], P('rows'), may hold values from 0 to 4095
Outputs:
- eigvecs: bfloat16 [40, 2097152], P('vecs', 'rows')
- residuals: bfloat16 [40, 2097152], P('vecs', 'rows')
- relative_norms: float32 [40], P('vecs')
The draws below stay inside these ranges and needn't reach their ends.
Inputs may be any that keep to these rules, and one draw needn't show every extreme that they name: Interface s joins subdomain s to subdomain (s + 1) mod 32; only its first link_count[s] slots are used, the others are to be ignored. Some interface uses all 4096 slots in every draw. `lower_cells`: slots beyond link_count[s] hold values that are not used. `upper_cells`: slots beyond link_count[s] hold values that are not used.
All inputs are finite; a program needn't handle non-finite values.
Results may differ from the reference program's by a relative error of at most 0.0037.
The reference program's roundings to bfloat16 on the way count: a program that leaves them out, or rounds other values in their place, can miss the bound.
Values may be sent and summed in bfloat16 or wider, within the bound.
No kernel may reach another device: no remote copies, remote signals or barrier semaphores. Data moves between devices by JAX's collectives and lax.ppermute only.
A program may use at most 320 MiB of HBM per device.

```python
import math
import jax
import jax.numpy as jnp
from jax import lax

RANK = 100
NV = 40
WID = 64
ZD = 16
HMAX = 4096
NSUB = 32
NROWS = 2097152
N_ROWS = 32


def draw_link_count(key, part):
    first_key, second_key = jax.random.split(jax.random.fold_in(key, 17))
    counts = jax.random.randint(first_key, (NSUB,), HMAX // 4, HMAX + 1)
    chosen = jax.random.randint(second_key, (), 0, NSUB)
    return jnp.where(jnp.arange(NSUB) == chosen, HMAX, counts).astype(jnp.int32)


def place_ends(array, key, least, largest):
    shape = array.shape
    place = [jax.random.randint(jax.random.fold_in(key, axis), (), 0, shape[axis]) for axis in range(len(shape))]
    array = array.at[tuple(place)].set(least)
    longest = shape.index(max(shape))
    place[longest] = (place[longest] + 1) % shape[longest]
    return array.at[tuple(place)].set(largest)


def block_levels(rng, dims, cuts, smallest, top_value):
    gain, own = 1.0, jax.random.fold_in(rng, 6)
    for dim, blocks in cuts:
        steps = jnp.exp(jax.random.uniform(jax.random.fold_in(own, dim), (blocks,), jnp.float32, smallest / len(cuts), top_value / len(cuts)))
        gain = gain * jnp.repeat(steps, dims[dim] // blocks).reshape([-1 if axis == dim else 1 for axis in range(len(dims))])
    return gain


def scatter_about(stream_key, dims, deviation, reach, cuts=(), held_as=jnp.bfloat16):
    result = deviation * jax.random.normal(stream_key, dims, jnp.float32)
    if cuts:
        result = result * block_levels(stream_key, dims, cuts, -0.22, 0.18)
    return jnp.clip(result, -reach, reach).astype(held_as)


def setup_inputs(seed: int = 0) -> dict:
    keys = jax.random.split(jax.random.key(seed), 10)
    basis = scatter_about(keys[0], (RANK, NROWS), 1.0, 6.0, ((0, 4), (1, 32)))
    coefficients = scatter_about(keys[1], (RANK, NV), RANK ** -0.5, 0.625)
    eigen_values = jnp.clip(-3.0 + 4.0 * jax.random.uniform(keys[2], (NV,), jnp.float32) ** block_levels(keys[2], (NV,), ((0, 4),), -0.2, 0.2), -3.0, 1.0)
    stiffness = jnp.clip(6.5 + 3.5 * jax.random.uniform(keys[3], (NROWS,), jnp.float32) ** block_levels(keys[3], (NROWS,), ((0, 32),), -0.2, 0.2), 6.5, 10.0)
    damping = jnp.clip(0.2 + 1.8 * jax.random.uniform(keys[4], (NROWS,), jnp.float32) ** block_levels(keys[4], (NROWS,), ((0, 32),), -0.2, 0.2), 0.2, 2.0)
    mass = jnp.clip(jnp.exp(math.log(2.0) - 1.3862944 * jax.random.uniform(keys[5], (NROWS,), jnp.float32) ** block_levels(keys[5], (NROWS,), ((0, 32),), -0.2, 0.2)), 0.5, 2.0)
    link_count = draw_link_count(jax.random.fold_in(keys[9], 71), 0)
    lower_cells = place_ends(jax.random.randint(keys[7], (NSUB, HMAX), 0, WID * WID), jax.random.fold_in(keys[7], 1), 0, (WID * WID) - 1).astype(jnp.int32)
    upper_cells = place_ends(jax.random.randint(keys[8], (NSUB, HMAX), 0, WID * WID), jax.random.fold_in(keys[8], 1), 0, (WID * WID) - 1).astype(jnp.int32)
    return {"basis": basis, "coefficients": coefficients, "eigen_values": eigen_values, "stiffness": stiffness, "damping": damping, "mass": mass, "link_count": link_count, "lower_cells": lower_cells, "upper_cells": upper_cells}


def neighbours(values, width_cells):
    depth_pad = jnp.pad(values, ((0, 0), (1, 1), (0, 0)))
    total = depth_pad[:, 2:] + depth_pad[:, :-2]
    across = jnp.pad(values, ((0, 0), (0, 0), (width_cells, width_cells)))
    total = total + across[:, :, 2 * width_cells:] + across[:, :, :-2 * width_cells]
    column = jnp.arange(values.shape[2]) % width_cells
    shifted = jnp.pad(values, ((0, 0), (0, 0), (1, 1)))
    total = total + jnp.where(column < width_cells - 1, shifted[:, :, 2:], 0.0)
    total = total + jnp.where(column > 0, shifted[:, :, :-2], 0.0)
    return total

def reference(basis, coefficients, eigen_values, stiffness, damping, mass, link_count, lower_cells, upper_cells):
    eigvecs = jnp.dot(coefficients.T, basis, preferred_element_type=jnp.float32).astype(jnp.bfloat16)
    vectors = eigvecs.astype(jnp.float32)
    plane_cells = WID * WID
    rows_local = ZD * plane_cells
    subdomains = N_ROWS
    neighbour_sum = neighbours(vectors.reshape(NV * subdomains, ZD, plane_cells), WID).reshape(NV, subdomains * rows_local)
    index_sub = jnp.arange(subdomains, dtype=jnp.int32)[:, None]
    lower_rows = (index_sub * rows_local + (ZD - 1) * plane_cells + lower_cells).reshape(-1).astype(jnp.int32)
    upper_rows = ((index_sub + 1) % subdomains * rows_local + upper_cells).reshape(-1).astype(jnp.int32)
    slot_used = (jnp.arange(HMAX, dtype=jnp.int32)[None, :] < link_count[:, None]).astype(jnp.float32).reshape(-1)
    link_sum = jnp.zeros_like(vectors)
    link_sum = link_sum.at[:, lower_rows].add(vectors[:, upper_rows] * slot_used)
    link_sum = link_sum.at[:, upper_rows].add(vectors[:, lower_rows] * slot_used)
    eigen_col = eigen_values[:, None]
    diagonal = eigen_col * eigen_col * mass[None, :] + eigen_col * damping[None, :] + stiffness[None, :]
    coupling = eigen_col * eigen_col * 0.1 + eigen_col * 0.3 + 1.0
    residual_full = diagonal * vectors - coupling * (neighbour_sum + link_sum)
    vector_sq = lax.optimization_barrier(jnp.sum(vectors * vectors, axis=1))
    residual_sq = lax.optimization_barrier(jnp.sum(residual_full * residual_full, axis=1))
    relative_norms = jnp.sqrt(residual_sq) / jnp.sqrt(vector_sq + 1.0)
    return (eigvecs, residual_full.astype(jnp.bfloat16), relative_norms)
```

```python
import functools

import jax
import jax.numpy as jnp
import numpy as np
from jax import lax
from jax.experimental import pallas as pl
from jax.experimental.pallas import tpu as pltpu
from jax.sharding import PartitionSpec as P

WID = 64
LANES = 128
SEGS = 8
NP = 16
BF = jnp.bfloat16
F32 = jnp.float32


def from_behind(value, axis, steps):
    count = lax.axis_size(axis)
    pairs = [(source, (source + steps) % count) for source in range(count)]
    return lax.ppermute(value, axis, pairs)


def cost(flops, nbytes):
    return pl.CostEstimate(flops=int(flops), bytes_accessed=int(nbytes), transcendentals=0)


def pack_kernel(starts, width, basis_ref, out_ref, buf, obuf, sem_in, sem_out):
    ranks = basis_ref.shape[0]
    full = ranks // 8 * 8
    rest = ranks - full
    seg = width // SEGS
    reads = [
        pltpu.make_async_copy(basis_ref.at[:, pl.ds(st, width)], buf.at[v], sem_in.at[v])
        for v, st in enumerate(starts)
    ]
    writes = [
        pltpu.make_async_copy(obuf.at[v], out_ref.at[v], sem_out.at[v]) for v in range(len(starts))
    ]
    for r in reads:
        r.start()
    for v in range(len(starts)):
        reads[v].wait()
        for c in range(SEGS):
            obuf[v, c * full : (c + 1) * full, :] = buf[v, 0:full, c * seg : (c + 1) * seg]
        tail = [buf[v, full:ranks, c * seg : (c + 1) * seg] for c in range(SEGS)]
        obuf[v, SEGS * full : SEGS * ranks, :] = jnp.concatenate(tail, axis=0)
        if v > 0:
            writes[v - 1].start()
    writes[-1].start()
    for w in writes:
        w.wait()


def pack(basis, starts, width):
    ranks = basis.shape[0]
    n = len(starts)
    seg = width // SEGS
    return pl.pallas_call(
        functools.partial(pack_kernel, starts, width),
        out_shape=jax.ShapeDtypeStruct((n, SEGS * ranks, seg), BF),
        in_specs=[pl.BlockSpec(memory_space=pl.ANY)],
        out_specs=pl.BlockSpec(memory_space=pl.ANY),
        scratch_shapes=[
            pltpu.VMEM((n, ranks, width), BF),
            pltpu.VMEM((n, SEGS * ranks, seg), BF),
            pltpu.SemaphoreType.DMA((n,)),
            pltpu.SemaphoreType.DMA((n,)),
        ],
        cost_estimate=cost(0, 4 * n * ranks * width),
        name="pack",
    )(basis)


def row_orders(parts, ranks, vecs):
    full = ranks // 8 * 8
    rest = ranks - full
    vfull = vecs // 8 * 8
    vrest = vecs - vfull
    col_rank, col_seg = [], []
    for s in range(parts):
        for c in range(SEGS):
            for r in range(full):
                col_rank.append(s * ranks + r)
                col_seg.append(c)
        for c in range(SEGS):
            for r in range(rest):
                col_rank.append(s * ranks + full + r)
                col_seg.append(c)
    row_vec, row_seg = [], []
    for v in range(parts):
        for c in range(SEGS):
            for j in range(vfull):
                row_vec.append(v * vecs + j)
                row_seg.append(c)
        for c in range(SEGS):
            for j in range(vrest):
                row_vec.append(v * vecs + vfull + j)
                row_seg.append(c)
    return [np.array(a, np.int32) for a in (col_rank, col_seg, row_vec, row_seg)]


def spread_kernel(coef_ref, cr_ref, cs_ref, rv_ref, rs_ref, out_ref):
    total, vecs = coef_ref.shape
    cols, rows = cr_ref.shape[1], rv_ref.shape[0]
    pick_rank = (lax.broadcasted_iota(jnp.int32, (total, cols), 0) == cr_ref[...]).astype(F32).astype(BF)
    pick_vec = (lax.broadcasted_iota(jnp.int32, (rows, vecs), 1) == rv_ref[...]).astype(F32).astype(BF)
    by_row = lax.dot_general(
        pick_vec, coef_ref[...], (((1,), (1,)), ((), ())), preferred_element_type=F32
    ).astype(BF)
    spread = jnp.dot(by_row, pick_rank, preferred_element_type=F32)
    out_ref[...] = jnp.where(rs_ref[...] == cs_ref[...], spread, 0.0).astype(BF)


def spread_coefficients(coefficients, parts, ranks, vecs):
    cr, cs, rv, rs = row_orders(parts, ranks, vecs)
    return pl.pallas_call(
        spread_kernel,
        out_shape=jax.ShapeDtypeStruct((rv.size, cr.size), BF),
        cost_estimate=cost(2 * rv.size * cr.size * parts * ranks, 2 * rv.size * cr.size),
        name="spread",
    )(
        coefficients,
        jnp.asarray(cr)[None, :],
        jnp.asarray(cs)[None, :],
        jnp.asarray(rv)[:, None],
        jnp.asarray(rs)[:, None],
    )


def mix_kernel(l_ref, y_ref, out_ref):
    out_ref[...] = jnp.dot(l_ref[...], y_ref[...], preferred_element_type=F32).astype(BF)


def mix(spread, packed):
    rows, depth = spread.shape
    lanes = packed.shape[1]
    step = 256
    return pl.pallas_call(
        mix_kernel,
        out_shape=jax.ShapeDtypeStruct((rows, lanes), BF),
        grid=(lanes // step,),
        in_specs=[
            pl.BlockSpec((rows, depth), lambda i: (0, 0)),
            pl.BlockSpec((depth, step), lambda i: (0, i)),
        ],
        out_specs=pl.BlockSpec((rows, step), lambda i: (0, i)),
        cost_estimate=cost(2 * rows * depth * lanes, 2 * (rows + depth) * lanes),
        name="mix",
    )(spread, packed)


def link_kernel(plane_ref, g_ref, s_ref, n_ref, out_ref, hot_s, put):
    nd, rows2, low = plane_ref.shape
    slots = g_ref.shape[2]
    half_rows = rows2 // 2
    vfull, vrest = 8, half_rows // SEGS - 8
    step = 512
    for d in range(nd):

        def build(i, _):
            at = pl.ds(pl.multiple_of(i * step, step), step)
            lane = lax.broadcasted_iota(jnp.int32, (low, step), 0)
            g = g_ref[d, :, at]
            s = s_ref[d, :, at]
            slot = lax.broadcasted_iota(jnp.int32, (1, step), 1) + i * step
            used = slot < n_ref[d]
            hot_g = jnp.where(lane == jnp.bitwise_and(g, low - 1), 1.0, 0.0).astype(BF)
            got = jnp.dot(plane_ref[d], hot_g, preferred_element_type=F32)
            gh = lax.shift_right_logical(g, 8)
            sh = jnp.where(used, lax.shift_right_logical(s, 8), -1)
            main = jnp.zeros((vfull, step), F32)
            tail = jnp.zeros((SEGS * vrest, step), F32)
            tail_seg = lax.broadcasted_iota(jnp.int32, (SEGS * vrest, step), 0) // vrest
            for h in range(2):
                base = h * half_rows
                for c in range(SEGS):
                    part = got[base + c * vfull : base + (c + 1) * vfull]
                    main = main + jnp.where(gh == h * SEGS + c, part, 0.0)
                part = got[base + SEGS * vfull : base + half_rows]
                tail = tail + jnp.where(gh == tail_seg + h * SEGS, part, 0.0)
            same = lax.broadcasted_iota(jnp.int32, (SEGS * vrest, SEGS * vrest), 0) % vrest == (
                lax.broadcasted_iota(jnp.int32, (SEGS * vrest, SEGS * vrest), 1) % vrest
            )
            tail = jnp.dot(
                jnp.where(same, 1.0, 0.0).astype(BF), tail.astype(BF), preferred_element_type=F32
            )
            pieces = []
            for h in range(2):
                for c in range(SEGS):
                    pieces.append(jnp.where(sh == h * SEGS + c, main, 0.0))
                pieces.append(jnp.where(sh == tail_seg + h * SEGS, tail, 0.0))
            put[:, at] = jnp.concatenate(pieces, axis=0).astype(BF)
            hot_s[:, at] = jnp.where(lane == jnp.bitwise_and(s, low - 1), 1.0, 0.0).astype(BF)
            return 0

        lax.fori_loop(0, slots // step, build, 0)
        total = lax.dot_general(
            put[...], hot_s[...], (((1,), (1,)), ((), ())), preferred_element_type=F32
        )
        for h in range(2):
            base = h * half_rows
            for c in range(SEGS):
                for k in range(low // LANES):
                    t = d * 32 + (h * SEGS + c) * (low // LANES) + k
                    at = slice(k * LANES, (k + 1) * LANES)
                    out_ref[t, 0:8, :] = total[base + c * 8 : base + (c + 1) * 8, at]
                    first = base + SEGS * 8 + c * vrest
                    out_ref[t, 8 : 8 + vrest, :] = total[first : first + vrest, at]


def link_terms(plane, g, s, n):
    nd, rows2, low = plane.shape
    slots = g.shape[2]
    return pl.pallas_call(
        link_kernel,
        out_shape=jax.ShapeDtypeStruct((nd * 32, NP, LANES), F32),
        in_specs=[
            pl.BlockSpec(memory_space=pltpu.VMEM),
            pl.BlockSpec(memory_space=pltpu.VMEM),
            pl.BlockSpec(memory_space=pltpu.VMEM),
            pl.BlockSpec(memory_space=pltpu.SMEM),
        ],
        out_specs=pl.BlockSpec(memory_space=pltpu.VMEM),
        scratch_shapes=[
            pltpu.VMEM((low, slots), BF),
            pltpu.VMEM((rows2, slots), BF),
        ],
        cost_estimate=cost(nd * 4 * rows2 * low * slots, nd * 4 * rows2 * low),
        name="links",
    )(plane, g, s, n)


def residual_kernel(
    chunks, planes, z_refs, link_ref, eig_ref, stiff_ref, damp_ref, mass_ref,
    vec_ref, res_ref, sum_ref, cells
):
    tiles = WID * WID // LANES
    vecs = vec_ref.shape[0]
    vrest = vecs - 8
    lane = lax.broadcasted_iota(jnp.int32, (1, LANES), 1)
    low_half = lane < WID
    column = jnp.bitwise_and(lane, WID - 1)
    not_first, not_last = column > 0, column < WID - 1
    blank = jnp.zeros((tiles, NP, LANES), F32)
    cells[0:tiles] = blank
    cells[(planes + 1) * tiles : (planes + 2) * tiles] = blank
    for (starts, width), z_ref in zip(chunks, z_refs):
        seg = width // SEGS
        for v, st in enumerate(starts):
            for c in range(SEGS):
                for k in range(seg // LANES):
                    t = (st + c * seg) // LANES + k
                    at = slice(k * LANES, (k + 1) * LANES)
                    top = z_ref[v, c * 8 : (c + 1) * 8, at]
                    first = SEGS * 8 + c * vrest
                    low = z_ref[v, first : first + vrest, at]
                    cells[tiles + t, 0:8, :] = top.astype(F32)
                    cells[tiles + t, 8 : 8 + vrest, :] = low.astype(F32)
    eig = jnp.concatenate([eig_ref[...], jnp.zeros((NP - vecs, 1), F32)], axis=0)
    eig = jnp.broadcast_to(eig, (NP, LANES))
    eig_sq = eig * eig
    coupling = eig_sq * 0.1 + eig * 0.3 + 1.0

    def plane(z, carry, link):
        vsum, rsum = carry
        base = pl.multiple_of((z + 1) * tiles, tiles)
        for i in range(tiles):
            x = cells[base + i]
            ahead = cells[base + i + 1] if i + 1 < tiles else None
            behind = cells[base + i - 1] if i > 0 else None
            if behind is None:
                across = jnp.where(low_half, ahead, 0.0)
            elif ahead is None:
                across = jnp.where(low_half, 0.0, behind)
            else:
                across = jnp.where(low_half, ahead, behind)
            total = pltpu.roll(x + across, WID, 1)
            total = total + jnp.where(not_first, pltpu.roll(x, 1, 1), 0.0)
            total = total + jnp.where(not_last, pltpu.roll(x, LANES - 1, 1), 0.0)
            total = total + (cells[base + i - tiles] + cells[base + i + tiles])
            if link is not None:
                total = total + link_ref[link * tiles + i]
            row = pl.ds(z * tiles + i, 1)
            diagonal = eig_sq * mass_ref[row, :] + eig * damp_ref[row, :] + stiff_ref[row, :]
            res = diagonal * x - coupling * total
            at = pl.ds(pl.multiple_of(z * WID * WID + i * LANES, LANES), LANES)
            vec_ref[:, at] = x[:vecs].astype(BF)
            res_ref[:, at] = res[:vecs].astype(BF)
            vsum = vsum + x * x
            rsum = rsum + res * res
        return vsum, rsum

    zero = jnp.zeros((NP, LANES), F32)
    carry = plane(0, (zero, zero), 0)
    carry = lax.fori_loop(1, planes - 1, lambda z, c: plane(z, c, None), carry)
    vsum, rsum = plane(planes - 1, carry, 1)
    vrow = jnp.broadcast_to(jnp.sum(vsum, axis=1, keepdims=True), (NP, LANES))
    rrow = jnp.broadcast_to(jnp.sum(rsum, axis=1, keepdims=True), (NP, LANES))
    sub = lax.broadcasted_iota(jnp.int32, (NP, LANES), 0)
    wide = lax.broadcasted_iota(jnp.int32, (NP, LANES), 1)
    both = jnp.where((sub == wide) & (sub < vecs), vrow, 0.0)
    both = both + jnp.where((sub + NP == wide) & (sub < vecs), rrow, 0.0)
    line = jnp.sum(both, axis=0, keepdims=True)
    sum_ref[...] = jnp.broadcast_to(line[None], sum_ref.shape)


def residual(chunks, zs, link, eig, stiff, damp, mass, vecs, rows_local, copies):
    planes = rows_local // (WID * WID)
    nz = len(zs)
    tiles = WID * WID // LANES

    def kernel(*refs):
        residual_kernel(chunks, planes, refs[:nz], *refs[nz:])

    return pl.pallas_call(
        kernel,
        out_shape=(
            jax.ShapeDtypeStruct((vecs, rows_local), BF),
            jax.ShapeDtypeStruct((vecs, rows_local), BF),
            jax.ShapeDtypeStruct((copies, 1, LANES), F32),
        ),
        in_specs=[pl.BlockSpec(memory_space=pltpu.VMEM)] * (nz + 5),
        out_specs=(pl.BlockSpec(memory_space=pltpu.VMEM),) * 3,
        scratch_shapes=[pltpu.VMEM(((planes + 2) * tiles, NP, LANES), F32)],
        cost_estimate=cost(40 * NP * rows_local, 8 * NP * rows_local),
        name="residual",
    )(*zs, link, eig, stiff, damp, mass)


def on_device(
    basis,
    coefficients,
    eigen_values,
    stiffness,
    damping,
    mass,
    link_count,
    lower_cells,
    upper_cells,
):
    parts = lax.axis_size("vecs")
    subdomains = lax.axis_size("rows")
    vecs = eigen_values.shape[0]
    ranks, rows_local = basis.shape
    plane = WID * WID
    planes = rows_local // plane
    half = plane // 2
    inner = (planes - 2) * plane // parts
    chunks = [
        ((0, half, (planes - 1) * plane, (planes - 1) * plane + half), half),
        (tuple(plane + v * inner for v in range(parts)), inner),
    ]
    down_lower, down_upper, down_count = from_behind(
        (lower_cells, upper_cells, link_count), "rows", 1
    )
    spread = spread_coefficients(coefficients, parts, ranks, vecs)
    packed = [pack(basis, starts, width) for starts, width in chunks]
    arrived = [lax.all_to_all(p, "vecs", 0, 0, tiled=True) for p in packed]
    mixed = [
        mix(spread, a.reshape(parts * SEGS * ranks, -1)).reshape(parts, SEGS * vecs, -1)
        for a in arrived
    ]
    back = [lax.all_to_all(m, "vecs", 0, 0, tiled=True) for m in mixed]
    ends = back[0].reshape(2, 2 * SEGS * vecs, -1)
    from_below = from_behind(ends[1:2], "rows", 1)
    from_above = from_behind(ends[0:1], "rows", -1)
    link = link_terms(
        jnp.concatenate([from_below, from_above], axis=0),
        jnp.stack([down_lower, upper_cells]),
        jnp.stack([down_upper, lower_cells]),
        jnp.concatenate([down_count, link_count]),
    )
    as_tiles = lambda a: a.reshape(rows_local // LANES, LANES)
    eigvecs, residuals, sums = residual(
        chunks, back, link, eigen_values[:, None], as_tiles(stiffness), as_tiles(damping),
        as_tiles(mass), vecs, rows_local, subdomains,
    )
    total = lax.all_to_all(sums, "rows", 0, 0, tiled=True).sum(axis=(0, 1))
    vector_sq, residual_sq = total[:vecs], total[NP : NP + vecs]
    relative_norms = jnp.sqrt(residual_sq) / jnp.sqrt(vector_sq + 1.0)
    return (eigvecs, residuals, relative_norms)


def solution(mesh):
    placed = (
        P("vecs", "rows"),
        P(),
        P("vecs"),
        P("rows"),
        P("rows"),
        P("rows"),
        P("rows"),
        P("rows", None),
        P("rows", None),
    )
    return jax.shard_map(
        on_device,
        mesh=mesh,
        in_specs=placed,
        out_specs=(P("vecs", "rows"), P("vecs", "rows"), P("vecs")),
        check_vma=False,
    )
```

```python
import functools

import jax
import jax.numpy as jnp
import numpy as np
from jax import lax
from jax.experimental import pallas as pl
from jax.experimental.pallas import tpu as pltpu
from jax.sharding import PartitionSpec as P

WID = 64
LANES = 128
SEGS = 8
NP = 16
BF = jnp.bfloat16
F32 = jnp.float32


def from_behind(value, axis, steps):
    count = lax.axis_size(axis)
    pairs = [(source, (source + steps) % count) for source in range(count)]
    return lax.ppermute(value, axis, pairs)


ANY = pl.BlockSpec(memory_space=pl.ANY)
VMEM = pl.BlockSpec(memory_space=pltpu.VMEM)
SMEM = pl.BlockSpec(memory_space=pltpu.SMEM)


def params(mib):
    return pltpu.CompilerParams(vmem_limit_bytes=mib * 1024 * 1024)


def cost(flops, nbytes):
    return pl.CostEstimate(flops=int(flops), bytes_accessed=int(nbytes), transcendentals=0)


class Chunk:
    def __init__(self, first, count, parts, planes):
        self.ends = first is None
        self.first = 0 if self.ends else first
        self.count = 2 if self.ends else count
        self.width = self.count * WID * WID // parts
        self.seg = self.width // SEGS
        self.jump = (planes - 2) * WID * WID if self.ends else 0
        self.parts = parts

    def start(self, v):
        base = self.first * WID * WID + v * self.width
        return base + jnp.where(2 * v >= self.parts, self.jump, 0) if self.ends else base


def pack_kernel(group, parts, me_ref, basis_ref, *rest):
    outs, (buf, sem) = rest[:parts], rest[parts:]
    ranks = basis_ref.shape[0]
    full = ranks // 8 * 8
    me = me_ref[0]
    reads = []
    for k in range(parts):
        v = lax.rem(me + k, parts)
        lane = 0
        for i, chunk in enumerate(group):
            st = pl.multiple_of(chunk.start(v), LANES)
            reads.append(
                pltpu.make_async_copy(
                    basis_ref.at[:, pl.ds(st, chunk.width)],
                    buf.at[k, :, pl.ds(lane, chunk.width)],
                    sem.at[k, i],
                )
            )
            lane += chunk.width
    for r in reads:
        r.start()
    for k in range(parts):
        lane, at = 0, 0
        for i, chunk in enumerate(group):
            reads[k * len(group) + i].wait()
            seg = chunk.seg
            tail = []
            for c in range(SEGS):
                cut = slice(lane + c * seg, lane + (c + 1) * seg)
                outs[k][c * full : (c + 1) * full, at : at + seg] = buf[k, 0:full, cut]
                tail.append(buf[k, full:ranks, cut])
            outs[k][SEGS * full : SEGS * ranks, at : at + seg] = jnp.concatenate(tail, axis=0)
            lane += chunk.width
            at += seg


def pack(me, basis, group, parts):
    ranks = basis.shape[0]
    seg = sum(chunk.seg for chunk in group)
    return pl.pallas_call(
        functools.partial(pack_kernel, group, parts),
        out_shape=[jax.ShapeDtypeStruct((SEGS * ranks, seg), BF)] * parts,
        in_specs=[SMEM, ANY],
        out_specs=[VMEM] * parts,
        scratch_shapes=[
            pltpu.VMEM((parts, ranks, SEGS * seg), BF),
            pltpu.SemaphoreType.DMA((parts, len(group))),
        ],
        compiler_params=params(60),
        cost_estimate=cost(1, 4 * parts * ranks * SEGS * seg),
        name="pack",
    )(me, basis)


def row_orders(ranks, vecs):
    full, vfull = ranks // 8 * 8, vecs // 8 * 8
    cols = [(r, c) for c in range(SEGS) for r in range(full)]
    cols += [(r, c) for c in range(SEGS) for r in range(full, ranks)]
    rows = [(j, c) for c in range(SEGS) for j in range(vfull)]
    rows += [(j, c) for c in range(SEGS) for j in range(vfull, vecs)]
    return np.array(cols, np.int32), np.array(rows, np.int32)


def spread_kernel(parts, me_ref, coef_ref, cr_ref, cs_ref, rv_ref, rs_ref, out_ref):
    total, wide = coef_ref.shape
    ranks, vecs = total // parts, wide // parts
    cols, rows = cr_ref.shape[1], rv_ref.shape[0]
    me = me_ref[0]
    coef = coef_ref[...]
    same = rs_ref[...] == cs_ref[...]
    for k in range(parts):
        source = lax.rem(me - k + parts, parts) * ranks
        pick = lax.broadcasted_iota(jnp.int32, (total, cols), 0) == cr_ref[...] + source
        by_col = lax.dot_general(
            coef, jnp.where(pick, 1.0, 0.0).astype(BF), (((0,), (0,)), ((), ())),
            preferred_element_type=F32,
        ).astype(BF)
        for o in range(parts):
            owner = lax.rem(me + o, parts) * vecs
            pick = lax.broadcasted_iota(jnp.int32, (rows, wide), 1) == rv_ref[...] + owner
            block = jnp.dot(
                jnp.where(pick, 1.0, 0.0).astype(BF), by_col, preferred_element_type=F32
            )
            out_ref[k, o * rows : (o + 1) * rows, :] = jnp.where(same, block, 0.0).astype(BF)


def spread_coefficients(me, coefficients, parts, ranks, vecs):
    cols, rows = row_orders(ranks, vecs)
    nc, nr = cols.shape[0], rows.shape[0]
    return pl.pallas_call(
        functools.partial(spread_kernel, parts),
        out_shape=jax.ShapeDtypeStruct((parts, parts * nr, nc), BF),
        in_specs=[SMEM] + [VMEM] * 5,
        out_specs=VMEM,
        compiler_params=params(8),
        cost_estimate=cost(20 * parts * parts * nr * nc, 2 * parts * parts * nr * nc),
        name="spread",
    )(
        me,
        coefficients,
        jnp.asarray(cols[:, 0])[None, :],
        jnp.asarray(cols[:, 1])[None, :],
        jnp.asarray(rows[:, 0])[:, None],
        jnp.asarray(rows[:, 1])[:, None],
    )


def mix_kernel(parts, lane, seg, l_ref, *rest):
    ys, outs = rest[:parts], rest[parts:]
    rows = outs[0].shape[0]
    step = 256

    def body(i, _):
        at = pl.multiple_of(i * step, step)
        total = None
        for k in range(parts):
            part = jnp.dot(
                l_ref[k], ys[k][:, pl.ds(lane + at, step)], preferred_element_type=F32
            )
            total = part if total is None else total + part
        for o in range(parts):
            outs[o][:, pl.ds(at, step)] = total[o * rows : (o + 1) * rows].astype(BF)
        return 0

    lax.fori_loop(0, seg // step, body, 0)


def mix(spread, packed, lane, seg, vecs):
    parts, rows, depth = spread.shape
    return pl.pallas_call(
        functools.partial(mix_kernel, parts, lane, seg),
        out_shape=[jax.ShapeDtypeStruct((SEGS * vecs, seg), BF)] * parts,
        in_specs=[VMEM] * (1 + parts),
        out_specs=[VMEM] * parts,
        compiler_params=params(12),
        cost_estimate=cost(2 * rows * parts * depth * seg, 2 * (rows + parts * depth) * seg),
        name="mix",
    )(spread, *packed)


def link_kernel(plane_ref, g_ref, s_ref, n_ref, out_ref, hot_s, put):
    nd, rows2, low = plane_ref.shape
    slots = g_ref.shape[2]
    half_rows = rows2 // 2
    vfull, vrest = 8, half_rows // SEGS - 8
    step = 512
    for d in range(nd):

        def build(i, _):
            at = pl.ds(pl.multiple_of(i * step, step), step)
            lane = lax.broadcasted_iota(jnp.int32, (low, step), 0)
            g = g_ref[d, :, at]
            s = s_ref[d, :, at]
            slot = lax.broadcasted_iota(jnp.int32, (1, step), 1) + i * step
            used = slot < n_ref[d]
            hot_g = jnp.where(lane == jnp.bitwise_and(g, low - 1), 1.0, 0.0).astype(BF)
            got = jnp.dot(plane_ref[d], hot_g, preferred_element_type=F32)
            gh = lax.shift_right_logical(g, 8)
            sh = jnp.where(used, lax.shift_right_logical(s, 8), -1)
            main = jnp.zeros((vfull, step), F32)
            tail = jnp.zeros((SEGS * vrest, step), F32)
            tail_seg = lax.broadcasted_iota(jnp.int32, (SEGS * vrest, step), 0) // vrest
            for h in range(2):
                base = h * half_rows
                for c in range(SEGS):
                    part = got[base + c * vfull : base + (c + 1) * vfull]
                    main = main + jnp.where(gh == h * SEGS + c, part, 0.0)
                part = got[base + SEGS * vfull : base + half_rows]
                tail = tail + jnp.where(gh == tail_seg + h * SEGS, part, 0.0)
            same = lax.broadcasted_iota(jnp.int32, (SEGS * vrest, SEGS * vrest), 0) % vrest == (
                lax.broadcasted_iota(jnp.int32, (SEGS * vrest, SEGS * vrest), 1) % vrest
            )
            tail = jnp.dot(
                jnp.where(same, 1.0, 0.0).astype(BF), tail.astype(BF), preferred_element_type=F32
            )
            pieces = []
            for h in range(2):
                for c in range(SEGS):
                    pieces.append(jnp.where(sh == h * SEGS + c, main, 0.0))
                pieces.append(jnp.where(sh == tail_seg + h * SEGS, tail, 0.0))
            put[:, at] = jnp.concatenate(pieces, axis=0).astype(BF)
            hot_s[:, at] = jnp.where(lane == jnp.bitwise_and(s, low - 1), 1.0, 0.0).astype(BF)
            return 0

        lax.fori_loop(0, slots // step, build, 0)
        total = lax.dot_general(
            put[...], hot_s[...], (((1,), (1,)), ((), ())), preferred_element_type=F32
        )
        for h in range(2):
            base = h * half_rows
            for c in range(SEGS):
                for k in range(low // LANES):
                    t = d * 32 + (h * SEGS + c) * (low // LANES) + k
                    at = slice(k * LANES, (k + 1) * LANES)
                    out_ref[t, 0:8, :] = total[base + c * 8 : base + (c + 1) * 8, at]
                    first = base + SEGS * 8 + c * vrest
                    out_ref[t, 8 : 8 + vrest, :] = total[first : first + vrest, at]


def link_terms(plane, g, s, n):
    nd, rows2, low = plane.shape
    slots = g.shape[2]
    return pl.pallas_call(
        link_kernel,
        out_shape=jax.ShapeDtypeStruct((nd * 32, NP, LANES), F32),
        in_specs=[
            pl.BlockSpec(memory_space=pltpu.VMEM),
            pl.BlockSpec(memory_space=pltpu.VMEM),
            pl.BlockSpec(memory_space=pltpu.VMEM),
            pl.BlockSpec(memory_space=pltpu.SMEM),
        ],
        out_specs=pl.BlockSpec(memory_space=pltpu.VMEM),
        scratch_shapes=[
            pltpu.VMEM((low, slots), BF),
            pltpu.VMEM((rows2, slots), BF),
        ],
        compiler_params=params(12),
        cost_estimate=cost(nd * 4 * rows2 * low * slots, nd * 4 * rows2 * low),
        name="links",
    )(plane, g, s, n)


def unpack(cells, tile0, chunk, me, parts, z_refs, vrest):
    for k in range(parts):
        first = chunk.start(lax.rem(me - k + parts, parts)) // LANES - tile0
        per = chunk.seg // LANES
        for c in range(SEGS):
            for i in range(per):
                at = slice(i * LANES, (i + 1) * LANES)
                t = first + c * per + i
                low = SEGS * 8 + c * vrest
                cells[t, 0:8, :] = z_refs[k][c * 8 : (c + 1) * 8, at].astype(F32)
                cells[t, 8 : 8 + vrest, :] = z_refs[k][low : low + vrest, at].astype(F32)


class Terms:
    def __init__(self, eig_ref, stiff_ref, damp_ref, mass_ref):
        vecs = eig_ref.shape[0]
        eig = jnp.concatenate([eig_ref[...], jnp.zeros((NP - vecs, 1), F32)], axis=0)
        self.eig = jnp.broadcast_to(eig, (NP, LANES))
        self.eig_sq = self.eig * self.eig
        self.coupling = self.eig_sq * 0.1 + self.eig * 0.3 + 1.0
        self.diagonals = (stiff_ref, damp_ref, mass_ref)
        lane = lax.broadcasted_iota(jnp.int32, (1, LANES), 1)
        self.low_half = lane < WID
        column = jnp.bitwise_and(lane, WID - 1)
        self.not_first, self.not_last = column > 0, column < WID - 1


def one_plane(terms, cells, z, z0, carry, link, outs):
    tiles = WID * WID // LANES
    vsum, rsum = carry
    base = (z - z0) * tiles
    stiff_ref, damp_ref, mass_ref = terms.diagonals
    for i in range(tiles):
        x = cells[base + i]
        ahead = cells[base + i + 1] if i + 1 < tiles else None
        behind = cells[base + i - 1] if i > 0 else None
        if behind is None:
            across = jnp.where(terms.low_half, ahead, 0.0)
        elif ahead is None:
            across = jnp.where(terms.low_half, 0.0, behind)
        else:
            across = jnp.where(terms.low_half, ahead, behind)
        total = pltpu.roll(x + across, WID, 1)
        total = total + jnp.where(terms.not_first, pltpu.roll(x, 1, 1), 0.0)
        total = total + jnp.where(terms.not_last, pltpu.roll(x, LANES - 1, 1), 0.0)
        if link is None:
            total = total + (cells[base + i - tiles] + cells[base + i + tiles])
        else:
            link_ref, offset, side = link
            total = total + (link_ref[offset + i] + cells[base + i + side * tiles])
        row = pl.ds(z * tiles + i, 1)
        diagonal = (
            terms.eig_sq * mass_ref[row, :] + terms.eig * damp_ref[row, :] + stiff_ref[row, :]
        )
        res = diagonal * x - terms.coupling * total
        if outs is not None:
            vec_ref, res_ref, o0 = outs
            vecs = vec_ref.shape[0]
            at = pl.ds(pl.multiple_of(z * WID * WID - o0 + i * LANES, LANES), LANES)
            vec_ref[:, at] = x[:vecs].astype(BF)
            res_ref[:, at] = res[:vecs].astype(BF)
        vsum = vsum + x * x
        rsum = rsum + res * res
    return vsum, rsum


def early_kernel(
    chunks, parts, split, me_ref, *rest
):
    nz = parts * len(chunks)
    z_refs, rest = rest[:nz], rest[nz:]
    link_ref, eig_ref, stiff_ref, damp_ref, mass_ref = rest[:5]
    vec_ref, res_ref, edge_ref, sum_ref, cells, vec_buf, res_buf, sem = rest[5:]
    tiles = WID * WID // LANES
    vecs = vec_ref.shape[0]
    me = me_ref[0]
    for i, chunk in enumerate(chunks):
        unpack(cells, 0, chunk, me, parts, z_refs[i * parts : (i + 1) * parts], vecs - 8)
    terms = Terms(eig_ref, stiff_ref, damp_ref, mass_ref)
    zero = jnp.zeros((NP, LANES), F32)
    outs = (vec_buf, res_buf, 0)
    carry = one_plane(terms, cells, 0, 0, (zero, zero), (link_ref, 0, 1), outs)
    carry = lax.fori_loop(
        1, split, lambda z, c: one_plane(terms, cells, z, 0, c, None, outs), carry
    )
    sum_ref[0], sum_ref[1] = carry
    edge_ref[0 : 2 * tiles] = cells[(split - 1) * tiles : (split + 1) * tiles]
    edge_ref[2 * tiles : 3 * tiles] = cells[cells.shape[0] - tiles : cells.shape[0]]
    at = pl.ds(0, split * WID * WID)
    copies = [
        pltpu.make_async_copy(vec_buf, vec_ref.at[:, at], sem.at[0]),
        pltpu.make_async_copy(res_buf, res_ref.at[:, at], sem.at[1]),
    ]
    for c in copies:
        c.start()
    for c in copies:
        c.wait()


def early(me, chunks, zs, link, eig, diagonals, vecs, rows_local, parts, split):
    tiles = WID * WID // LANES
    planes = rows_local // (WID * WID)
    lanes = split * WID * WID
    return pl.pallas_call(
        functools.partial(early_kernel, chunks, parts, split),
        out_shape=(
            jax.ShapeDtypeStruct((vecs, rows_local), BF),
            jax.ShapeDtypeStruct((vecs, rows_local), BF),
            jax.ShapeDtypeStruct((3 * tiles, NP, LANES), F32),
            jax.ShapeDtypeStruct((2, NP, LANES), F32),
        ),
        in_specs=[SMEM] + [VMEM] * (len(zs) + 5),
        out_specs=(ANY, ANY, VMEM, VMEM),
        scratch_shapes=[
            pltpu.VMEM((planes * tiles, NP, LANES), F32),
            pltpu.VMEM((vecs, lanes), BF),
            pltpu.VMEM((vecs, lanes), BF),
            pltpu.SemaphoreType.DMA((2,)),
        ],
        compiler_params=params(24),
        cost_estimate=cost(4000 * NP * lanes, 8 * NP * lanes),
        name="early",
    )(me, *zs, link, eig, *diagonals)


def late_planes(chunk, parts, split, planes, me_ref, z_refs, refs, cells, outs):
    edge_ref, link_ref, eig_ref, stiff_ref, damp_ref, mass_ref = refs
    tiles = WID * WID // LANES
    z0 = split - 1
    cells[0 : 2 * tiles] = edge_ref[0 : 2 * tiles]
    cells[(planes - 1 - z0) * tiles : (planes - z0) * tiles] = edge_ref[2 * tiles : 3 * tiles]
    unpack(cells, z0 * tiles, chunk, me_ref[0], parts, z_refs, eig_ref.shape[0] - 8)
    terms = Terms(eig_ref, stiff_ref, damp_ref, mass_ref)
    zero = jnp.zeros((NP, LANES), F32)
    carry = lax.fori_loop(
        split,
        planes - 1,
        lambda z, c: one_plane(terms, cells, z, z0, c, None, outs),
        (zero, zero),
    )
    return one_plane(terms, cells, planes - 1, z0, carry, (link_ref, tiles, -1), outs)


def sums_kernel(chunk, parts, split, planes, me_ref, *rest):
    z_refs, refs = rest[:parts], rest[parts : parts + 6]
    early_ref, out_ref, cells = rest[parts + 6 :]
    vecs = refs[2].shape[0]
    vsum, rsum = late_planes(chunk, parts, split, planes, me_ref, z_refs, refs, cells, None)
    vsum, rsum = vsum + early_ref[0], rsum + early_ref[1]
    vrow = jnp.broadcast_to(jnp.sum(vsum, axis=1, keepdims=True), (NP, LANES))
    rrow = jnp.broadcast_to(jnp.sum(rsum, axis=1, keepdims=True), (NP, LANES))
    sub = lax.broadcasted_iota(jnp.int32, (NP, LANES), 0)
    wide = lax.broadcasted_iota(jnp.int32, (NP, LANES), 1)
    both = jnp.where((sub == wide) & (sub < vecs), vrow, 0.0)
    both = both + jnp.where((sub + NP == wide) & (sub < vecs), rrow, 0.0)
    line = jnp.sum(both, axis=0, keepdims=True)
    out_ref[...] = jnp.broadcast_to(line[None], out_ref.shape)


def late_kernel(chunk, parts, split, planes, me_ref, *rest):
    z_refs, refs = rest[:parts], rest[parts : parts + 6]
    _, _, vec_ref, res_ref, cells, vec_buf, res_buf, sem = rest[parts + 6 :]
    o0 = split * WID * WID
    late_planes(chunk, parts, split, planes, me_ref, z_refs, refs, cells, (vec_buf, res_buf, o0))
    at = pl.ds(o0, vec_buf.shape[1])
    copies = [
        pltpu.make_async_copy(vec_buf, vec_ref.at[:, at], sem.at[0]),
        pltpu.make_async_copy(res_buf, res_ref.at[:, at], sem.at[1]),
    ]
    for c in copies:
        c.start()
    for c in copies:
        c.wait()


def late(me, chunk, zs, edge, link, eig, diagonals, sums, vec, res, parts, split, copies):
    vecs, rows_local = vec.shape
    planes = rows_local // (WID * WID)
    tiles = WID * WID // LANES
    lanes = (planes - split) * WID * WID
    cells = pltpu.VMEM(((planes - split + 1) * tiles, NP, LANES), F32)
    total = pl.pallas_call(
        functools.partial(sums_kernel, chunk, parts, split, planes),
        out_shape=jax.ShapeDtypeStruct((copies, 1, LANES), F32),
        in_specs=[SMEM] + [VMEM] * (parts + 7),
        out_specs=VMEM,
        scratch_shapes=[cells],
        compiler_params=params(16),
        cost_estimate=cost(4000 * NP * lanes, 8 * NP * lanes),
        name="sums",
    )(me, *zs, edge, link, eig, *diagonals, sums)
    first = 1 + parts + 6
    vec, res = pl.pallas_call(
        functools.partial(late_kernel, chunk, parts, split, planes),
        out_shape=(
            jax.ShapeDtypeStruct(vec.shape, vec.dtype),
            jax.ShapeDtypeStruct(res.shape, res.dtype),
        ),
        in_specs=[SMEM] + [VMEM] * (parts + 6) + [ANY, ANY],
        out_specs=(ANY, ANY),
        scratch_shapes=[
            cells,
            pltpu.VMEM((vecs, lanes), BF),
            pltpu.VMEM((vecs, lanes), BF),
            pltpu.SemaphoreType.DMA((2,)),
        ],
        input_output_aliases={first: 0, first + 1: 1},
        compiler_params=params(20),
        cost_estimate=cost(4000 * NP * lanes, 8 * NP * lanes),
        name="late",
    )(me, *zs, edge, link, eig, *diagonals, vec, res)
    return total, vec, res


def exchanged(arrays, axis):
    return [arrays[0]] + [from_behind(arrays[k], axis, k) for k in range(1, len(arrays))]


def on_device(
    basis,
    coefficients,
    eigen_values,
    stiffness,
    damping,
    mass,
    link_count,
    lower_cells,
    upper_cells,
):
    parts = lax.axis_size("vecs")
    subdomains = lax.axis_size("rows")
    vecs = eigen_values.shape[0]
    ranks, rows_local = basis.shape
    slots = lower_cells.shape[1]
    planes = rows_local // (WID * WID)
    me = lax.axis_index("vecs").astype(jnp.int32)[None]
    split = 10
    ends = Chunk(None, 2, parts, planes)
    first = Chunk(1, split, parts, planes)
    second = Chunk(1 + split, planes - 2 - split, parts, planes)
    lists = jnp.concatenate(
        [lower_cells, upper_cells, jnp.broadcast_to(link_count[:, None], (1, LANES))], axis=1
    )
    ends_out = exchanged(pack(me, basis, [ends], parts), "vecs")
    inner_out = exchanged(pack(me, basis, [first, second], parts), "vecs")
    down = from_behind(lists, "rows", 1)
    spread = spread_coefficients(me, coefficients, parts, ranks, vecs)
    z_ends = exchanged(mix(spread, ends_out, 0, ends.seg, vecs), "vecs")
    both = lambda a, b: jnp.stack([a, b])
    by_source = lambda v: lax.dynamic_index_in_dim(
        jnp.stack(z_ends), lax.rem(me[0] - v + parts, parts), 0, keepdims=False
    )
    plane_low = jnp.concatenate([by_source(0), by_source(1)], axis=0)
    plane_high = jnp.concatenate([by_source(2), by_source(3)], axis=0)
    from_below = from_behind(plane_high, "rows", 1)
    from_above = from_behind(plane_low, "rows", -1)
    link = link_terms(
        both(from_below, from_above),
        both(down[:, :slots], upper_cells),
        both(down[:, slots : 2 * slots], lower_cells),
        jnp.concatenate([down[0, 2 * slots : 2 * slots + 1], link_count]),
    )
    inner_out[0], link = lax.optimization_barrier((inner_out[0], link))
    z_first = exchanged(mix(spread, inner_out, 0, first.seg, vecs), "vecs")
    z_second = exchanged(mix(spread, inner_out, first.seg, second.seg, vecs), "vecs")
    diagonals = [a.reshape(rows_local // LANES, LANES) for a in (stiffness, damping, mass)]
    eig = eigen_values[:, None]
    vec, res, edge, sums = early(
        me, [ends, first], z_ends + z_first, link, eig, diagonals, vecs, rows_local, parts, split
    )
    sums, vec, res = late(
        me, second, z_second, edge, link, eig, diagonals, sums, vec, res, parts, split, subdomains
    )
    total = lax.all_to_all(sums, "rows", 0, 0, tiled=True).sum(axis=(0, 1))
    vector_sq, residual_sq = total[:vecs], total[NP : NP + vecs]
    relative_norms = jnp.sqrt(residual_sq) / jnp.sqrt(vector_sq + 1.0)
    return (vec, res, relative_norms)


def solution(mesh):
    placed = (
        P("vecs", "rows"),
        P(),
        P("vecs"),
        P("rows"),
        P("rows"),
        P("rows"),
        P("rows"),
        P("rows", None),
        P("rows", None),
    )
    return jax.shard_map(
        on_device,
        mesh=mesh,
        in_specs=placed,
        out_specs=(P("vecs", "rows"), P("vecs", "rows"), P("vecs")),
        check_vma=False,
    )
```

```python
import functools

import jax
import jax.numpy as jnp
from jax import lax
from jax.experimental import pallas as pl
from jax.experimental.pallas import tpu as pltpu
from jax.sharding import PartitionSpec as P


WID = 64
LANES = 128
SEGS = 8
NP = 16
BF = jnp.bfloat16
F32 = jnp.float32


def from_behind(value, axis, steps):
    count = lax.axis_size(axis)
    pairs = [(source, (source + steps) % count) for source in range(count)]
    return lax.ppermute(value, axis, pairs)


ANY = pl.BlockSpec(memory_space=pl.ANY)
VMEM = pl.BlockSpec(memory_space=pltpu.VMEM)
SMEM = pl.BlockSpec(memory_space=pltpu.SMEM)


def params(mib):
    return pltpu.CompilerParams(vmem_limit_bytes=mib * 1024 * 1024)


def cost(flops, nbytes):
    return pl.CostEstimate(flops=int(flops), bytes_accessed=int(nbytes), transcendentals=0)


class Chunk:
    def __init__(self, first, count, parts, planes):
        self.first = first or 0
        self.width = count * WID * WID // parts
        self.seg = self.width // SEGS
        self.jump = (planes - count) * WID * WID if first is None else 0
        self.parts = parts

    def start(self, v):
        base = self.first * WID * WID + v * self.width
        return base + jnp.where(2 * v >= self.parts, self.jump, 0) if self.jump else base


class Packing:
    def __init__(self, chunk, parts, me, basis_ref, outs, buf, sem):
        self.chunk, self.outs, self.buf, self.reads = chunk, outs, buf, []
        for k in range(parts):
            st = pl.multiple_of(chunk.start(lax.rem(me + k, parts)), LANES)
            read = pltpu.make_async_copy(
                basis_ref.at[:, pl.ds(st, chunk.width)], buf.at[k], sem.at[k]
            )
            read.start()
            self.reads.append(read)

    def finish(self):
        ranks, seg = self.buf.shape[1], self.chunk.seg
        full = ranks // 8 * 8
        for read, out, k in zip(self.reads, self.outs, range(len(self.outs))):
            read.wait()
            tail = []
            for c in range(SEGS):
                cut = slice(c * seg, (c + 1) * seg)
                out[c * full : (c + 1) * full, :] = self.buf[k, 0:full, cut]
                tail.append(self.buf[k, full:ranks, cut])
            out[SEGS * full : SEGS * ranks, :] = jnp.concatenate(tail, axis=0)


def packed_shape(chunk, ranks):
    return jax.ShapeDtypeStruct((SEGS * ranks, chunk.seg), BF)


def pack_scratch(chunk, ranks, parts):
    return [pltpu.VMEM((parts, ranks, chunk.width), BF), pltpu.SemaphoreType.DMA((parts,))]


def pack_kernel(chunk, parts, me_ref, basis_ref, *rest):
    Packing(chunk, parts, me_ref[0], basis_ref, rest[:parts], *rest[parts:]).finish()


def pack(me, basis, chunk, parts):
    ranks = basis.shape[0]
    return list(
        pl.pallas_call(
            functools.partial(pack_kernel, chunk, parts),
            out_shape=[packed_shape(chunk, ranks)] * parts,
            in_specs=[SMEM, ANY],
            out_specs=[VMEM] * parts,
            scratch_shapes=pack_scratch(chunk, ranks, parts),
            compiler_params=params(60),
            cost_estimate=cost(1, 4 * parts * ranks * chunk.width),
            name="pack",
        )(me, basis)
    )


def orders(shape, axis, main, rest):
    i = lax.broadcasted_iota(jnp.int32, shape, axis)
    body, tail = i < main * SEGS, i - main * SEGS
    entry = jnp.where(body, lax.rem(i, main), main + lax.rem(tail, rest))
    return entry, jnp.where(body, lax.div(i, main), lax.div(tail, rest))


def spread(parts, me, coef_ref, out_ref):
    wide, total = coef_ref.shape
    ranks, vecs = total // parts, wide // parts
    rows, cols = out_ref.shape[1] // parts, out_ref.shape[2]
    full, vfull = ranks // 8 * 8, vecs // 8 * 8
    col_rank, col_seg = orders((1, cols), 1, full, ranks - full)
    row_vec, row_seg = orders((rows, 1), 0, vfull, vecs - vfull)
    coef = coef_ref[...]
    same = row_seg == col_seg
    for k in range(parts):
        source = lax.rem(me - k + parts, parts) * ranks
        pick = lax.broadcasted_iota(jnp.int32, (total, cols), 0) == col_rank + source
        by_col = jnp.dot(
            coef, jnp.where(pick, 1.0, 0.0).astype(BF), preferred_element_type=F32
        ).astype(BF)
        for o in range(parts):
            owner = lax.rem(me + o, parts) * vecs
            pick = lax.broadcasted_iota(jnp.int32, (rows, wide), 1) == row_vec + owner
            block = jnp.dot(
                jnp.where(pick, 1.0, 0.0).astype(BF), by_col, preferred_element_type=F32
            )
            out_ref[k, o * rows : (o + 1) * rows, :] = jnp.where(same, block, 0.0).astype(BF)


def spread_coefficients(me, coefficients, parts, ranks, vecs):
    nc, nr = SEGS * ranks, SEGS * vecs
    return pl.pallas_call(
        lambda me_ref, coef_ref, out_ref: spread(parts, me_ref[0], coef_ref, out_ref),
        out_shape=jax.ShapeDtypeStruct((parts, parts * nr, nc), BF),
        in_specs=[SMEM, VMEM],
        out_specs=VMEM,
        compiler_params=params(8),
        cost_estimate=cost(20 * parts * parts * nr * nc, 2 * parts * parts * nr * nc),
        name="spread",
    )(me, coefficients.T)


def mix_kernel(parts, lane, seg, l_ref, *rest):
    ys, outs = rest[:parts], rest[parts:]
    rows = outs[0].shape[0]
    step = 256

    def body(at, step):
        total = None
        for k in range(parts):
            part = jnp.dot(
                l_ref[k], ys[k][:, pl.ds(lane + at, step)], preferred_element_type=F32
            )
            total = part if total is None else total + part
        for o in range(parts):
            outs[o][:, pl.ds(at, step)] = total[o * rows : (o + 1) * rows].astype(BF)

    @pl.loop(0, seg // step)
    def _(i):
        body(pl.multiple_of(i * step, step), step)

    if seg % step:
        body(seg // step * step, seg % step)


def mix(matrix, packed, lane, seg, vecs):
    parts, rows, depth = matrix.shape
    return pl.pallas_call(
        functools.partial(mix_kernel, parts, lane, seg),
        out_shape=[jax.ShapeDtypeStruct((SEGS * vecs, seg), BF)] * parts,
        in_specs=[VMEM] * (1 + parts),
        out_specs=[VMEM] * parts,
        compiler_params=params(12),
        cost_estimate=cost(2 * rows * parts * depth * seg, 2 * (rows + parts * depth) * seg),
        name="mix",
    )(matrix, *packed)


def one_hot_kernel(low, down_ref, lower_ref, upper_ref, count_ref, g_ref, s_ref, seg_ref):
    slots = lower_ref.shape[1]
    shift = low.bit_length() - 1
    step = 256
    lane = lax.broadcasted_iota(jnp.int32, (low, 1), 0)
    across = lax.broadcasted_iota(jnp.int32, (1, low), 1)
    ways = (
        (down_ref, 0, down_ref, slots, down_ref[:, 2 * slots : 2 * slots + 1]),
        (upper_ref, 0, lower_ref, 0, count_ref[...]),
    )

    @pl.loop(0, slots // step)
    def _(i):
        at = pl.ds(pl.multiple_of(i * step, step), step)
        slot = lax.broadcasted_iota(jnp.int32, (1, step), 1) + i * step
        for d, (from_ref, f0, to_ref, t0, count) in enumerate(ways):
            g = from_ref[:, pl.ds(pl.multiple_of(f0 + i * step, step), step)]
            s = to_ref[:, pl.ds(pl.multiple_of(t0 + i * step, step), step)]
            g_low, s_low = jnp.bitwise_and(g, low - 1), jnp.bitwise_and(s, low - 1)
            g_ref[d, :, at] = jnp.where(lane == g_low, 1.0, 0.0).astype(BF)
            for j in range(0, step, LANES):
                down_sub = jnp.broadcast_to(s_low[:, j : j + LANES], (LANES, LANES)).T
                down_sub = jnp.concatenate([down_sub] * (low // LANES), axis=1)
                rows = pl.ds(pl.multiple_of(i * step + j, LANES), LANES)
                s_ref[d, rows, :] = jnp.where(down_sub == across, 1.0, 0.0).astype(BF)
            seg_ref[2 * d : 2 * d + 1, at] = lax.shift_right_logical(g, shift)
            seg_ref[2 * d + 1 : 2 * d + 2, at] = jnp.where(
                slot < count, lax.shift_right_logical(s, shift), -1
            )


def one_hots(low, down, lower, upper, count):
    slots = lower.shape[1]
    hot = jax.ShapeDtypeStruct((2, low, slots), BF)
    hot_down = jax.ShapeDtypeStruct((2, slots, low), BF)
    return pl.pallas_call(
        functools.partial(one_hot_kernel, low),
        out_shape=(hot, hot_down, jax.ShapeDtypeStruct((4, slots), jnp.int32)),
        in_specs=[VMEM] * 4,
        out_specs=[VMEM] * 3,
        compiler_params=params(20),
        cost_estimate=cost(40 * low * slots, 8 * low * slots),
        name="one_hots",
    )(down, lower, upper, count)


def link_kernel(below_ref, above_ref, g_ref, s_ref, seg_ref, out_ref, put):
    rows, low = below_ref.shape
    slots = g_ref.shape[2]
    vfull = 8
    vrest = rows // SEGS - vfull
    step = 512
    tail_rows = SEGS * vrest
    tail_seg = lax.broadcasted_iota(jnp.int32, (tail_rows, 1), 0) // vrest
    for i in range(slots // step):
        at = slice(i * step, (i + 1) * step)
        for d, plane_ref in enumerate((below_ref, above_ref)):
            got = jnp.dot(plane_ref[...], g_ref[d, :, at], preferred_element_type=F32)
            gh, sh = seg_ref[2 * d : 2 * d + 1, at], seg_ref[2 * d + 1 : 2 * d + 2, at]
            main = got[0:vfull]
            for c in range(1, SEGS):
                main = jnp.where(gh == c, got[c * vfull : (c + 1) * vfull], main)
            tail = jnp.where(gh == tail_seg, got[SEGS * vfull : rows], 0.0)
            shift = vrest
            while shift < tail_rows:
                tail = tail + pltpu.roll(tail, shift, 0)
                shift *= 2
            pieces = [jnp.where(sh == c, main, 0.0) for c in range(SEGS)]
            pieces.append(jnp.where(sh == tail_seg, tail, 0.0))
            put[d, :, at] = jnp.concatenate(pieces, axis=0).astype(BF)

    for d in range(2):
        total = jnp.dot(put[d], s_ref[d], preferred_element_type=F32)
        for c in range(SEGS):
            for k in range(low // LANES):
                t = d * 32 + c * (low // LANES) + k
                at = slice(k * LANES, (k + 1) * LANES)
                out_ref[t, 0:8, :] = total[c * 8 : (c + 1) * 8, at]
                first = SEGS * 8 + c * vrest
                out_ref[t, 8 : 8 + vrest, :] = total[first : first + vrest, at]


def link_terms(below, above, hots):
    rows, low = below.shape
    slots = hots[0].shape[2]
    return pl.pallas_call(
        link_kernel,
        out_shape=jax.ShapeDtypeStruct((64, NP, LANES), F32),
        in_specs=[VMEM] * 5,
        out_specs=VMEM,
        scratch_shapes=[pltpu.VMEM((2, rows, slots), BF)],
        compiler_params=params(10),
        cost_estimate=cost(8 * rows * low * slots, 8 * rows * low),
        name="links",
    )(below, above, *hots)


def ends_kernel(parts, me_ref, *rest):
    z_refs, (low_ref, high_ref) = rest[:parts], rest[parts:]
    for k in range(parts):
        v = lax.rem(me_ref[0] - k + parts, parts)

        @pl.when(v == 0)
        def _():
            low_ref[...] = z_refs[k][...]

        @pl.when(v == parts - 1)
        def _():
            high_ref[...] = z_refs[k][...]


def end_planes(me, zs):
    parts = len(zs)
    shape = jax.ShapeDtypeStruct(zs[0].shape, BF)
    return pl.pallas_call(
        functools.partial(ends_kernel, parts),
        out_shape=(shape, shape),
        in_specs=[SMEM] + [VMEM] * parts,
        out_specs=(VMEM, VMEM),
        compiler_params=params(8),
        cost_estimate=cost(1, 8 * zs[0].size * parts),
        name="ends",
    )(me, *zs)


def unpack(cells, tile0, chunk, me, parts, z_refs, vrest):
    for k in range(parts):
        first = chunk.start(lax.rem(me - k + parts, parts)) // LANES - tile0
        per = chunk.seg // LANES
        for c in range(SEGS):
            for i in range(per):
                at = slice(i * LANES, (i + 1) * LANES)
                t = first + c * per + i
                low = SEGS * 8 + c * vrest
                cells[t, 0:8, :] = z_refs[k][c * 8 : (c + 1) * 8, at].astype(F32)
                cells[t, 8 : 8 + vrest, :] = z_refs[k][low : low + vrest, at].astype(F32)


class Output:
    def __init__(self, refs, bufs, sem, low):
        self.refs, self.bufs, self.sem, self.low = refs, bufs, sem, low
        self.copies = []

    def send(self, first, last):
        lanes = (last - first) * WID * WID
        to = pl.ds(first * WID * WID, lanes)
        at = pl.ds((first - self.low) * WID * WID, lanes)
        for i in range(2):
            copy = pltpu.make_async_copy(
                self.bufs[i].at[:, at], self.refs[i].at[:, to], self.sem.at[len(self.copies)]
            )
            copy.start()
            self.copies.append(copy)

    def wait(self):
        for copy in self.copies:
            copy.wait()


def cuts(low, high, step=3):
    marks = list(range(low, high, step))
    return list(zip(marks, marks[1:] + [high]))


class Terms:
    def __init__(self, eig_ref, stiff_ref, damp_ref, mass_ref):
        vecs = eig_ref.shape[1]
        sub = lax.broadcasted_iota(jnp.int32, (NP, vecs), 0)
        own = sub == lax.broadcasted_iota(jnp.int32, (NP, vecs), 1)
        eig = jnp.sum(jnp.where(own, eig_ref[...], 0.0), axis=1, keepdims=True)
        self.eig = jnp.broadcast_to(eig, (NP, LANES))
        self.eig_sq = self.eig * self.eig
        self.coupling = self.eig_sq * 0.1 + self.eig * 0.3 + 1.0
        self.diagonals = (stiff_ref, damp_ref, mass_ref)
        lane = lax.broadcasted_iota(jnp.int32, (1, LANES), 1)
        self.low_half = lane < WID
        column = jnp.bitwise_and(lane, WID - 1)
        self.not_first, self.not_last = column > 0, column < WID - 1


def one_plane(terms, cells, z, z0, carry, link, outs):
    tiles = WID * WID // LANES
    vsum, rsum = carry
    base = (z - z0) * tiles
    stiff_ref, damp_ref, mass_ref = terms.diagonals
    for i in range(tiles):
        x = cells[base + i]
        ahead = cells[base + i + 1] if i + 1 < tiles else None
        behind = cells[base + i - 1] if i > 0 else None
        if behind is None:
            across = jnp.where(terms.low_half, ahead, 0.0)
        elif ahead is None:
            across = jnp.where(terms.low_half, 0.0, behind)
        else:
            across = jnp.where(terms.low_half, ahead, behind)
        total = pltpu.roll(x + across, WID, 1)
        total = total + jnp.where(terms.not_first, pltpu.roll(x, 1, 1), 0.0)
        total = total + jnp.where(terms.not_last, pltpu.roll(x, LANES - 1, 1), 0.0)
        if link is None:
            total = total + (cells[base + i - tiles] + cells[base + i + tiles])
        else:
            link_ref, offset, side = link
            total = total + (link_ref[offset + i] + cells[base + i + side * tiles])
        row = pl.ds(z * tiles + i, 1)
        diagonal = (
            terms.eig_sq * mass_ref[row, :] + terms.eig * damp_ref[row, :] + stiff_ref[row, :]
        )
        res = diagonal * x - terms.coupling * total
        if outs is not None:
            vec_ref, res_ref, o0 = outs
            vecs = vec_ref.shape[0]
            at = pl.ds(pl.multiple_of(z * WID * WID - o0 + i * LANES, LANES), LANES)
            vec_ref[:, at] = x[:vecs].astype(BF)
            res_ref[:, at] = res[:vecs].astype(BF)
        vsum = vsum + x * x
        rsum = rsum + res * res
    return vsum, rsum


def residual_kernel(chunks, parts, planes, me_ref, *rest):
    nz = parts * len(chunks)
    z_refs, rest = rest[:nz], rest[nz:]
    link_ref, eig_ref, stiff_ref, damp_ref, mass_ref = rest[:5]
    vec_ref, res_ref, out_ref, cells, vec_buf, res_buf, sem = rest[5:]
    vecs = vec_ref.shape[0]
    tiles = WID * WID // LANES
    for i, chunk in enumerate(chunks):
        unpack(cells, 0, chunk, me_ref[0], parts, z_refs[i * parts : (i + 1) * parts], vecs - 8)
    terms = Terms(eig_ref, stiff_ref, damp_ref, mass_ref)
    outs = (vec_buf, res_buf, 0)
    out = Output((vec_ref, res_ref), (vec_buf, res_buf), sem, 0)
    zero = jnp.zeros((NP, LANES), F32)
    carry = one_plane(terms, cells, 0, 0, (zero, zero), (link_ref, 0, 1), outs)
    carry = one_plane(terms, cells, planes - 1, 0, carry, (link_ref, tiles, -1), outs)
    ready = [(0, 1), (planes - 1, planes)]
    for first, end in cuts(1, planes - 1):
        carry = lax.fori_loop(
            first, end, lambda z, c: one_plane(terms, cells, z, 0, c, None, outs), carry
        )
        for cut in ready:
            out.send(*cut)
        ready = [(first, end)]
    vsum, rsum = carry
    vrow = jnp.broadcast_to(jnp.sum(vsum, axis=1, keepdims=True), (NP, LANES))
    rrow = jnp.broadcast_to(jnp.sum(rsum, axis=1, keepdims=True), (NP, LANES))
    sub = lax.broadcasted_iota(jnp.int32, (NP, LANES), 0)
    wide = lax.broadcasted_iota(jnp.int32, (NP, LANES), 1)
    both = jnp.where((sub == wide) & (sub < vecs), vrow, 0.0)
    both = both + jnp.where((sub + NP == wide) & (sub < vecs), rrow, 0.0)
    line = jnp.sum(both, axis=0, keepdims=True)
    out_ref[...] = jnp.broadcast_to(line[None], out_ref.shape)
    for cut in ready:
        out.send(*cut)
    out.wait()


def residual(me, chunks, zs, link, eig, diagonals, vecs, rows_local, parts, copies):
    planes = rows_local // (WID * WID)
    tiles = WID * WID // LANES
    whole = jax.ShapeDtypeStruct((vecs, rows_local), BF)
    return pl.pallas_call(
        functools.partial(residual_kernel, chunks, parts, planes),
        out_shape=(whole, whole, jax.ShapeDtypeStruct((copies, 1, LANES), F32)),
        in_specs=[SMEM] + [VMEM] * (len(zs) + 5),
        out_specs=(ANY, ANY, VMEM),
        scratch_shapes=[
            pltpu.VMEM((planes * tiles, NP, LANES), F32),
            pltpu.VMEM((vecs, rows_local), BF),
            pltpu.VMEM((vecs, rows_local), BF),
            pltpu.SemaphoreType.DMA((32,)),
        ],
        compiler_params=params(24),
        cost_estimate=cost(4000 * NP * rows_local, 8 * NP * rows_local),
        name="residual",
    )(me, *zs, link, eig, *diagonals)


def kept(value):
    def kernel(from_ref, to_ref):
        to_ref[...] = from_ref[...]

    return pl.pallas_call(
        kernel,
        out_shape=jax.ShapeDtypeStruct(value.shape, value.dtype),
        in_specs=[VMEM],
        out_specs=VMEM,
        compiler_params=params(4),
        cost_estimate=cost(1, 4 * value.size),
        name="kept",
    )(value)


def exchanged(arrays, axis):
    return [arrays[0]] + [from_behind(arrays[k], axis, k) for k in range(1, len(arrays))]


def on_device(
    basis,
    coefficients,
    eigen_values,
    stiffness,
    damping,
    mass,
    link_count,
    lower_cells,
    upper_cells,
):
    parts = lax.axis_size("vecs")
    subdomains = lax.axis_size("rows")
    vecs = eigen_values.shape[0]
    ranks, rows_local = basis.shape
    planes = rows_local // (WID * WID)
    me = lax.axis_index("vecs").astype(jnp.int32)[None]
    ends = Chunk(None, 4, parts, planes)
    inner = Chunk(2, planes - 4, parts, planes)
    wide_count = jnp.broadcast_to(link_count[:, None], (1, LANES))
    lists = jnp.concatenate([lower_cells, upper_cells, wide_count], axis=1)
    ends_out = pack(me, basis, ends, parts)
    ends_out = exchanged(ends_out, "vecs")
    inner_out = pack(me, basis, inner, parts)
    inner_out = exchanged(inner_out, "vecs")
    down = from_behind(lists, "rows", 1)
    matrix = spread_coefficients(me, coefficients, parts, ranks, vecs)
    hots = one_hots(ends.seg, down, lower_cells, upper_cells, wide_count[:, :1])
    inner_out[0] = kept(inner_out[0])
    z_ends = mix(matrix, ends_out, 0, ends.seg, vecs)
    z_ends = exchanged(z_ends, "vecs")
    z_inner = mix(matrix, inner_out, 0, inner.seg, vecs)
    z_inner = exchanged(z_inner, "vecs")
    plane_low, plane_high = end_planes(me, z_ends)
    from_below = from_behind(plane_high, "rows", 1)
    from_above = from_behind(plane_low, "rows", -1)
    link = link_terms(from_below, from_above, hots)
    diagonals = [a.reshape(rows_local // LANES, LANES) for a in (stiffness, damping, mass)]
    eigvecs, residuals, sums = residual(
        me, [ends, inner], z_ends + z_inner, link, eigen_values[None, :], diagonals, vecs,
        rows_local, parts, subdomains,
    )
    total = lax.all_to_all(sums, "rows", 0, 0, tiled=True).sum(axis=(0, 1))
    vector_sq, residual_sq = total[:vecs], total[NP : NP + vecs]
    relative_norms = jnp.sqrt(residual_sq) / jnp.sqrt(vector_sq + 1.0)
    return (eigvecs, residuals, relative_norms)


def solution(mesh):
    placed = (
        P("vecs", "rows"),
        P(),
        P("vecs"),
        P("rows"),
        P("rows"),
        P("rows"),
        P("rows"),
        P("rows", None),
        P("rows", None),
    )
    return jax.shard_map(
        on_device,
        mesh=mesh,
        in_specs=placed,
        out_specs=(P("vecs", "rows"), P("vecs", "rows"), P("vecs")),
        check_vma=False,
    )
```

```python
import functools

import jax
import jax.numpy as jnp
from jax import lax
from jax.experimental import pallas as pl
from jax.experimental.pallas import tpu as pltpu
from jax.sharding import PartitionSpec as P


WID = 64
LANES = 128
SEGS = 8
NP = 16
BF = jnp.bfloat16
F32 = jnp.float32


def from_behind(value, axis, steps):
    count = lax.axis_size(axis)
    pairs = [(source, (source + steps) % count) for source in range(count)]
    return lax.ppermute(value, axis, pairs)


ANY = pl.BlockSpec(memory_space=pl.ANY)
VMEM = pl.BlockSpec(memory_space=pltpu.VMEM)
SMEM = pl.BlockSpec(memory_space=pltpu.SMEM)


def params(mib):
    return pltpu.CompilerParams(vmem_limit_bytes=mib * 1024 * 1024)


def cost(flops, nbytes):
    return pl.CostEstimate(flops=int(flops), bytes_accessed=int(nbytes), transcendentals=0)


class Chunk:
    def __init__(self, first, count, parts, planes):
        self.first = first or 0
        self.width = count * WID * WID // parts
        self.seg = self.width // SEGS
        self.jump = (planes - count) * WID * WID if first is None else 0
        self.parts = parts

    def start(self, v):
        base = self.first * WID * WID + v * self.width
        return base + jnp.where(2 * v >= self.parts, self.jump, 0) if self.jump else base


class Packing:
    def __init__(self, chunk, parts, me, basis_ref, outs, buf, sem):
        self.chunk, self.outs, self.buf, self.reads = chunk, outs, buf, []
        for k in range(parts):
            st = pl.multiple_of(chunk.start(lax.rem(me + k, parts)), LANES)
            read = pltpu.make_async_copy(
                basis_ref.at[:, pl.ds(st, chunk.width)], buf.at[k], sem.at[k]
            )
            read.start()
            self.reads.append(read)

    def finish(self):
        ranks, seg = self.buf.shape[1], self.chunk.seg
        full = ranks // 8 * 8
        for read, out, k in zip(self.reads, self.outs, range(len(self.outs))):
            read.wait()
            tail = []
            for c in range(SEGS):
                cut = slice(c * seg, (c + 1) * seg)
                out[c * full : (c + 1) * full, :] = self.buf[k, 0:full, cut]
                tail.append(self.buf[k, full:ranks, cut])
            out[SEGS * full : SEGS * ranks, :] = jnp.concatenate(tail, axis=0)


def packed_shape(chunk, ranks):
    return jax.ShapeDtypeStruct((SEGS * ranks, chunk.seg), BF)


def pack_scratch(chunk, ranks, parts):
    return [pltpu.VMEM((parts, ranks, chunk.width), BF), pltpu.SemaphoreType.DMA((parts,))]


def pack_kernel(chunks, parts, me_ref, basis_ref, *rest):
    n = parts * len(chunks)
    outs, scratch = rest[:n], rest[n:]
    work = [
        Packing(
            chunk, parts, me_ref[0], basis_ref, outs[i * parts : (i + 1) * parts],
            *scratch[2 * i : 2 * i + 2]
        )
        for i, chunk in enumerate(chunks)
    ]
    for w in work:
        w.finish()


def pack(me, basis, chunks, parts):
    ranks = basis.shape[0]
    shapes, scratch = [], []
    for chunk in chunks:
        shapes += [packed_shape(chunk, ranks)] * parts
        scratch += pack_scratch(chunk, ranks, parts)
    packed = pl.pallas_call(
        functools.partial(pack_kernel, chunks, parts),
        out_shape=shapes,
        in_specs=[SMEM, ANY],
        out_specs=[VMEM] * len(shapes),
        scratch_shapes=scratch,
        compiler_params=params(60),
        cost_estimate=cost(1, 4 * parts * ranks * sum(chunk.width for chunk in chunks)),
        name="pack",
    )(me, basis)
    return [list(packed[i * parts : (i + 1) * parts]) for i in range(len(chunks))]


def orders(shape, axis, main, rest):
    i = lax.broadcasted_iota(jnp.int32, shape, axis)
    body, tail = i < main * SEGS, i - main * SEGS
    entry = jnp.where(body, lax.rem(i, main), main + lax.rem(tail, rest))
    return entry, jnp.where(body, lax.div(i, main), lax.div(tail, rest))


def spread(parts, me, coef_ref, out_ref):
    wide, total = coef_ref.shape
    ranks, vecs = total // parts, wide // parts
    rows, cols = out_ref.shape[1] // parts, out_ref.shape[2]
    full, vfull = ranks // 8 * 8, vecs // 8 * 8
    col_rank, col_seg = orders((1, cols), 1, full, ranks - full)
    row_vec, row_seg = orders((rows, 1), 0, vfull, vecs - vfull)
    coef = coef_ref[...]
    same = row_seg == col_seg
    for k in range(parts):
        source = lax.rem(me - k + parts, parts) * ranks
        pick = lax.broadcasted_iota(jnp.int32, (total, cols), 0) == col_rank + source
        by_col = jnp.dot(
            coef, jnp.where(pick, 1.0, 0.0).astype(BF), preferred_element_type=F32
        ).astype(BF)
        for o in range(parts):
            owner = lax.rem(me + o, parts) * vecs
            pick = lax.broadcasted_iota(jnp.int32, (rows, wide), 1) == row_vec + owner
            block = jnp.dot(
                jnp.where(pick, 1.0, 0.0).astype(BF), by_col, preferred_element_type=F32
            )
            out_ref[k, o * rows : (o + 1) * rows, :] = jnp.where(same, block, 0.0).astype(BF)


def spread_coefficients(me, coefficients, parts, ranks, vecs):
    nc, nr = SEGS * ranks, SEGS * vecs
    return pl.pallas_call(
        lambda me_ref, coef_ref, out_ref: spread(parts, me_ref[0], coef_ref, out_ref),
        out_shape=jax.ShapeDtypeStruct((parts, parts * nr, nc), BF),
        in_specs=[SMEM, VMEM],
        out_specs=VMEM,
        compiler_params=params(8),
        cost_estimate=cost(20 * parts * parts * nr * nc, 2 * parts * parts * nr * nc),
        name="spread",
    )(me, coefficients.T)


def mix_kernel(parts, lane, seg, l_ref, *rest):
    ys, outs = rest[:parts], rest[parts:]
    rows = outs[0].shape[0]
    step = 256

    def body(at, step):
        total = None
        for k in range(parts):
            part = jnp.dot(
                l_ref[k], ys[k][:, pl.ds(lane + at, step)], preferred_element_type=F32
            )
            total = part if total is None else total + part
        for o in range(parts):
            outs[o][:, pl.ds(at, step)] = total[o * rows : (o + 1) * rows].astype(BF)

    @pl.loop(0, seg // step)
    def _(i):
        body(pl.multiple_of(i * step, step), step)

    if seg % step:
        body(seg // step * step, seg % step)


def mix(matrix, packed, lane, seg, vecs):
    parts, rows, depth = matrix.shape
    return pl.pallas_call(
        functools.partial(mix_kernel, parts, lane, seg),
        out_shape=[jax.ShapeDtypeStruct((SEGS * vecs, seg), BF)] * parts,
        in_specs=[VMEM] * (1 + parts),
        out_specs=[VMEM] * parts,
        compiler_params=params(12),
        cost_estimate=cost(2 * rows * parts * depth * seg, 2 * (rows + parts * depth) * seg),
        name="mix",
    )(matrix, *packed)


def one_hot_kernel(low, down_ref, lower_ref, upper_ref, count_ref, g_ref, s_ref, seg_ref):
    slots = lower_ref.shape[1]
    shift = low.bit_length() - 1
    step = 256
    centred = lambda cells: (jnp.bitwise_and(cells, low - 1) - low // 2).astype(F32).astype(BF)
    lane = centred(lax.broadcasted_iota(jnp.int32, (low, step), 0))
    across = centred(lax.broadcasted_iota(jnp.int32, (LANES, low), 1))
    one, none = jnp.ones((), BF), jnp.zeros((), BF)
    ways = (
        (down_ref, 0, down_ref, slots, down_ref[:, 2 * slots : 2 * slots + 1]),
        (upper_ref, 0, lower_ref, 0, count_ref[...]),
    )

    @pl.loop(0, slots // step)
    def _(i):
        at = pl.ds(pl.multiple_of(i * step, step), step)
        slot = lax.broadcasted_iota(jnp.int32, (1, step), 1) + i * step
        for d, (from_ref, f0, to_ref, t0, count) in enumerate(ways):
            g = from_ref[:, pl.ds(pl.multiple_of(f0 + i * step, step), step)]
            s = to_ref[:, pl.ds(pl.multiple_of(t0 + i * step, step), step)]
            wanted = jnp.broadcast_to(centred(g), (low, step))
            g_ref[d, :, at] = jnp.where(lane == wanted, one, none)
            s_low = (jnp.bitwise_and(s, low - 1) - low // 2).astype(F32)
            for j in range(0, step, LANES):
                turned = jnp.broadcast_to(s_low[:, j : j + LANES], (LANES, LANES)).T.astype(BF)
                turned = jnp.concatenate([turned] * (low // LANES), axis=1)
                rows = pl.ds(pl.multiple_of(i * step + j, LANES), LANES)
                s_ref[d, rows, :] = jnp.where(turned == across, one, none)
            seg_ref[2 * d : 2 * d + 1, at] = lax.shift_right_logical(g, shift)
            seg_ref[2 * d + 1 : 2 * d + 2, at] = jnp.where(
                slot < count, lax.shift_right_logical(s, shift), -1
            )


def one_hots(low, down, lower, upper, count):
    slots = lower.shape[1]
    hot = jax.ShapeDtypeStruct((2, low, slots), BF)
    hot_down = jax.ShapeDtypeStruct((2, slots, low), BF)
    return pl.pallas_call(
        functools.partial(one_hot_kernel, low),
        out_shape=(hot, hot_down, jax.ShapeDtypeStruct((4, slots), jnp.int32)),
        in_specs=[VMEM] * 4,
        out_specs=[VMEM] * 3,
        compiler_params=params(20),
        cost_estimate=cost(40 * low * slots, 8 * low * slots),
        name="one_hots",
    )(down, lower, upper, count)


def link_kernel(below_ref, above_ref, g_ref, s_ref, seg_ref, out_ref, put):
    rows, wide = below_ref.shape
    low, slots = g_ref.shape[1:]
    per = wide // low
    vfull = 8
    vrest = rows // SEGS - vfull
    step = 512
    tail_rows = SEGS * vrest
    tail_seg = lax.broadcasted_iota(jnp.int32, (tail_rows, 1), 0) // vrest
    planes = [
        jnp.concatenate([ref[:, h * low : (h + 1) * low] for h in range(per)], axis=0)
        for ref in (below_ref, above_ref)
    ]
    for i in range(slots // step):
        at = slice(i * step, (i + 1) * step)
        for d, plane in enumerate(planes):
            got = jnp.dot(plane, g_ref[d, :, at], preferred_element_type=F32)
            gh, sh = seg_ref[2 * d : 2 * d + 1, at], seg_ref[2 * d + 1 : 2 * d + 2, at]
            main, tail = got[0:vfull], jnp.zeros((tail_rows, step), F32)
            for h in range(per):
                for c in range(SEGS):
                    part = got[h * rows + c * vfull : h * rows + (c + 1) * vfull]
                    main = jnp.where(gh == c * per + h, part, main)
                part = got[h * rows + SEGS * vfull : (h + 1) * rows]
                tail = jnp.where(gh == tail_seg * per + h, part, tail)
            shift = vrest
            while shift < tail_rows:
                tail = tail + pltpu.roll(tail, shift, 0)
                shift *= 2
            pieces = []
            for h in range(per):
                pieces += [jnp.where(sh == c * per + h, main, 0.0) for c in range(SEGS)]
                pieces.append(jnp.where(sh == tail_seg * per + h, tail, 0.0))
            put[d, :, at] = jnp.concatenate(pieces, axis=0).astype(BF)

    for d in range(2):
        total = jnp.dot(put[d], s_ref[d], preferred_element_type=F32)
        for h in range(per):
            for c in range(SEGS):
                for k in range(low // LANES):
                    t = d * 32 + (c * per + h) * (low // LANES) + k
                    at = slice(k * LANES, (k + 1) * LANES)
                    first = h * rows + c * 8
                    out_ref[t, 0:8, :] = total[first : first + 8, at]
                    first = h * rows + SEGS * 8 + c * vrest
                    out_ref[t, 8 : 8 + vrest, :] = total[first : first + vrest, at]


def link_terms(below, above, hots):
    rows = below.size // hots[0].shape[1]
    low, slots = hots[0].shape[1:]
    return pl.pallas_call(
        link_kernel,
        out_shape=jax.ShapeDtypeStruct((64, NP, LANES), F32),
        in_specs=[VMEM] * 5,
        out_specs=VMEM,
        scratch_shapes=[pltpu.VMEM((2, rows, slots), BF)],
        compiler_params=params(10),
        cost_estimate=cost(8 * rows * low * slots, 8 * rows * low),
        name="links",
    )(below, above, *hots)


def ends_kernel(parts, me_ref, *rest):
    z_refs, (low_ref, high_ref) = rest[:parts], rest[parts:]
    for k in range(parts):
        v = lax.rem(me_ref[0] - k + parts, parts)

        @pl.when(v == 0)
        def _():
            low_ref[...] = z_refs[k][...]

        @pl.when(v == parts - 1)
        def _():
            high_ref[...] = z_refs[k][...]


def end_planes(me, zs):
    parts = len(zs)
    shape = jax.ShapeDtypeStruct(zs[0].shape, BF)
    return pl.pallas_call(
        functools.partial(ends_kernel, parts),
        out_shape=(shape, shape),
        in_specs=[SMEM] + [VMEM] * parts,
        out_specs=(VMEM, VMEM),
        compiler_params=params(8),
        cost_estimate=cost(1, 8 * zs[0].size * parts),
        name="ends",
    )(me, *zs)


def unpack(cells, tile0, chunk, me, parts, z_refs, vrest):
    for k in range(parts):
        first = chunk.start(lax.rem(me - k + parts, parts)) // LANES - tile0
        per = chunk.seg // LANES
        for c in range(SEGS):
            for i in range(per):
                at = slice(i * LANES, (i + 1) * LANES)
                t = first + c * per + i
                low = SEGS * 8 + c * vrest
                cells[t, 0:8, :] = z_refs[k][c * 8 : (c + 1) * 8, at].astype(F32)
                cells[t, 8 : 8 + vrest, :] = z_refs[k][low : low + vrest, at].astype(F32)


class Output:
    def __init__(self, refs, bufs, sem, shifts):
        self.refs, self.bufs, self.sem, self.shifts = refs, bufs, sem, shifts
        self.copies = []

    def send(self, first, last):
        lanes = (last - first) * WID * WID
        to = pl.ds(first * WID * WID, lanes)
        shift = self.shifts.get(first, self.shifts.get(None, 0))
        at = pl.ds((first - shift) * WID * WID, lanes)
        for i in range(2):
            copy = pltpu.make_async_copy(
                self.bufs[i].at[:, at], self.refs[i].at[:, to], self.sem.at[len(self.copies)]
            )
            copy.start()
            self.copies.append(copy)

    def wait(self):
        for copy in self.copies:
            copy.wait()


def cuts(low, high, step=3):
    marks = list(range(low, high, step))
    return list(zip(marks, marks[1:] + [high]))


class Terms:
    def __init__(self, eig_ref, stiff_ref, damp_ref, mass_ref):
        vecs = eig_ref.shape[1]
        sub = lax.broadcasted_iota(jnp.int32, (NP, vecs), 0)
        own = sub == lax.broadcasted_iota(jnp.int32, (NP, vecs), 1)
        eig = jnp.sum(jnp.where(own, eig_ref[...], 0.0), axis=1, keepdims=True)
        self.eig = jnp.broadcast_to(eig, (NP, LANES))
        self.eig_sq = self.eig * self.eig
        self.coupling = self.eig_sq * 0.1 + self.eig * 0.3 + 1.0
        self.diagonals = (stiff_ref, damp_ref, mass_ref)
        lane = lax.broadcasted_iota(jnp.int32, (1, LANES), 1)
        self.low_half = lane < WID
        column = jnp.bitwise_and(lane, WID - 1)
        self.not_first, self.not_last = column > 0, column < WID - 1


def one_plane(terms, cells, z, z0, carry, link, outs):
    tiles = WID * WID // LANES
    vsum, rsum = carry
    base = (z - z0) * tiles
    stiff_ref, damp_ref, mass_ref = terms.diagonals
    for i in range(tiles):
        x = cells[base + i]
        ahead = cells[base + i + 1] if i + 1 < tiles else None
        behind = cells[base + i - 1] if i > 0 else None
        if behind is None:
            across = jnp.where(terms.low_half, ahead, 0.0)
        elif ahead is None:
            across = jnp.where(terms.low_half, 0.0, behind)
        else:
            across = jnp.where(terms.low_half, ahead, behind)
        total = pltpu.roll(x + across, WID, 1)
        total = total + jnp.where(terms.not_first, pltpu.roll(x, 1, 1), 0.0)
        total = total + jnp.where(terms.not_last, pltpu.roll(x, LANES - 1, 1), 0.0)
        if link is None:
            total = total + (cells[base + i - tiles] + cells[base + i + tiles])
        else:
            link_ref, offset, side = link
            total = total + (link_ref[offset + i] + cells[base + i + side * tiles])
        row = pl.ds(z * tiles + i, 1)
        diagonal = (
            terms.eig_sq * mass_ref[row, :] + terms.eig * damp_ref[row, :] + stiff_ref[row, :]
        )
        res = diagonal * x - terms.coupling * total
        if outs is not None:
            vec_ref, res_ref, o0 = outs
            vecs = vec_ref.shape[0]
            at = pl.ds(pl.multiple_of(z * WID * WID - o0 + i * LANES, LANES), LANES)
            vec_ref[:, at] = x[:vecs].astype(BF)
            res_ref[:, at] = res[:vecs].astype(BF)
        vsum = vsum + x * x
        rsum = rsum + res * res
    return vsum, rsum


def finished_planes(terms, cells, z0, carry, links, outs, out, low, high, ends):
    ready = []
    for z in ends:
        carry = one_plane(terms, cells, z, z0, carry, links.get(z), outs(z))
        ready.append((z, z + 1))
    for first, end in cuts(low, high):
        carry = lax.fori_loop(
            first, end, lambda z, c: one_plane(terms, cells, z, z0, c, None, outs(first)), carry
        )
        for cut in ready:
            out.send(*cut)
        ready = [(first, end)]
    return carry, ready


def part_one_kernel(chunks, parts, planes, split, me_ref, *rest):
    nz = parts * len(chunks)
    z_refs, rest = rest[:nz], rest[nz:]
    link_ref, eig_ref, stiff_ref, damp_ref, mass_ref = rest[:5]
    vec_ref, res_ref, edge_ref, sum_ref, cells, vec_buf, res_buf, sem = rest[5:]
    vecs = vec_ref.shape[0]
    tiles = WID * WID // LANES
    for i, chunk in enumerate(chunks):
        unpack(cells, 0, chunk, me_ref[0], parts, z_refs[i * parts : (i + 1) * parts], vecs - 8)
    terms = Terms(eig_ref, stiff_ref, damp_ref, mass_ref)
    moved = (planes - 1 - split) * WID * WID
    outs = lambda z: (vec_buf, res_buf, moved if z == planes - 1 else 0)
    out = Output((vec_ref, res_ref), (vec_buf, res_buf), sem, {planes - 1: planes - 1 - split})
    zero = jnp.zeros((NP, LANES), F32)
    links = {0: (link_ref, 0, 1), planes - 1: (link_ref, tiles, -1)}
    carry, ready = finished_planes(
        terms, cells, 0, (zero, zero), links, outs, out, 1, split, (0, planes - 1)
    )
    edge_ref[0 : 2 * tiles] = cells[(split - 1) * tiles : (split + 1) * tiles]
    edge_ref[2 * tiles : 4 * tiles] = cells[(planes - 2) * tiles : planes * tiles]
    sum_ref[0], sum_ref[1] = carry
    for cut in ready:
        out.send(*cut)
    out.wait()


def part_two_kernel(chunk, parts, planes, split, me_ref, *rest):
    z_refs, rest = rest[:parts], rest[parts:]
    edge_ref, eig_ref, stiff_ref, damp_ref, mass_ref, early_ref, _, _ = rest[:8]
    vec_ref, res_ref, out_ref, cells, vec_buf, res_buf, sem = rest[8:]
    vecs = vec_ref.shape[0]
    tiles = WID * WID // LANES
    z0 = split - 1
    cells[0 : 2 * tiles] = edge_ref[0 : 2 * tiles]
    cells[(planes - 2 - z0) * tiles : (planes - z0) * tiles] = edge_ref[2 * tiles : 4 * tiles]
    unpack(cells, z0 * tiles, chunk, me_ref[0], parts, z_refs, vecs - 8)
    terms = Terms(eig_ref, stiff_ref, damp_ref, mass_ref)
    outs = lambda z: (vec_buf, res_buf, split * WID * WID)
    out = Output((vec_ref, res_ref), (vec_buf, res_buf), sem, {None: split})
    carry = (early_ref[0], early_ref[1])
    carry, ready = finished_planes(terms, cells, z0, carry, {}, outs, out, split, planes - 1, ())
    vsum, rsum = carry
    vrow = jnp.broadcast_to(jnp.sum(vsum, axis=1, keepdims=True), (NP, LANES))
    rrow = jnp.broadcast_to(jnp.sum(rsum, axis=1, keepdims=True), (NP, LANES))
    sub = lax.broadcasted_iota(jnp.int32, (NP, LANES), 0)
    wide = lax.broadcasted_iota(jnp.int32, (NP, LANES), 1)
    both = jnp.where((sub == wide) & (sub < vecs), vrow, 0.0)
    both = both + jnp.where((sub + NP == wide) & (sub < vecs), rrow, 0.0)
    line = jnp.sum(both, axis=0, keepdims=True)
    out_ref[...] = jnp.broadcast_to(line[None], out_ref.shape)
    for cut in ready:
        out.send(*cut)
    out.wait()


def buffers(planes, kept_planes, vecs):
    tiles = WID * WID // LANES
    return [
        pltpu.VMEM((planes * tiles, NP, LANES), F32),
        pltpu.VMEM((vecs, kept_planes * WID * WID), BF),
        pltpu.VMEM((vecs, kept_planes * WID * WID), BF),
        pltpu.SemaphoreType.DMA((16,)),
    ]


def part_one(me, chunks, zs, link, eig, diagonals, vecs, rows_local, parts, split):
    planes = rows_local // (WID * WID)
    tiles = WID * WID // LANES
    whole = jax.ShapeDtypeStruct((vecs, rows_local), BF)
    return pl.pallas_call(
        functools.partial(part_one_kernel, chunks, parts, planes, split),
        out_shape=(
            whole,
            whole,
            jax.ShapeDtypeStruct((4 * tiles, NP, LANES), F32),
            jax.ShapeDtypeStruct((2, NP, LANES), F32),
        ),
        in_specs=[SMEM] + [VMEM] * (len(zs) + 5),
        out_specs=(ANY, ANY, VMEM, VMEM),
        scratch_shapes=buffers(planes, split + 1, vecs),
        compiler_params=params(20),
        cost_estimate=cost(2000 * NP * rows_local, 4 * NP * rows_local),
        name="part_one",
    )(me, *zs, link, eig, *diagonals)


def part_two(me, chunk, zs, edge, eig, diagonals, early, vec, res, parts, split, copies):
    vecs, rows_local = vec.shape
    planes = rows_local // (WID * WID)
    whole = jax.ShapeDtypeStruct((vecs, rows_local), BF)
    first = 1 + parts + 6
    return pl.pallas_call(
        functools.partial(part_two_kernel, chunk, parts, planes, split),
        out_shape=(whole, whole, jax.ShapeDtypeStruct((copies, 1, LANES), F32)),
        in_specs=[SMEM] + [VMEM] * (parts + 6) + [ANY, ANY],
        out_specs=(ANY, ANY, VMEM),
        scratch_shapes=buffers(planes - split + 1, planes - 1 - split, vecs),
        input_output_aliases={first: 0, first + 1: 1},
        compiler_params=params(20),
        cost_estimate=cost(2000 * NP * rows_local, 4 * NP * rows_local),
        name="part_two",
    )(me, *zs, edge, eig, *diagonals, early, vec, res)


def kept(value):
    def kernel(from_ref, to_ref):
        to_ref[...] = from_ref[...]

    return pl.pallas_call(
        kernel,
        out_shape=jax.ShapeDtypeStruct(value.shape, value.dtype),
        in_specs=[VMEM],
        out_specs=VMEM,
        compiler_params=params(4),
        cost_estimate=cost(1, 4 * value.size),
        name="kept",
    )(value)


def exchanged(arrays, axis):
    return [arrays[0]] + [from_behind(arrays[k], axis, k) for k in range(1, len(arrays))]


def on_device(
    basis,
    coefficients,
    eigen_values,
    stiffness,
    damping,
    mass,
    link_count,
    lower_cells,
    upper_cells,
):
    parts = lax.axis_size("vecs")
    subdomains = lax.axis_size("rows")
    vecs = eigen_values.shape[0]
    ranks, rows_local = basis.shape
    planes = rows_local // (WID * WID)
    me = lax.axis_index("vecs").astype(jnp.int32)[None]
    ends = Chunk(None, 4, parts, planes)
    middle = (planes - 4) // 2 + 2
    one = Chunk(2, middle - 2, parts, planes)
    two = Chunk(middle, planes - 2 - middle, parts, planes)
    wide_count = jnp.broadcast_to(link_count[:, None], (1, LANES))
    lists = jnp.concatenate([lower_cells, upper_cells, wide_count], axis=1)
    (ends_out,) = pack(me, basis, [ends], parts)
    ends_out = exchanged(ends_out, "vecs")
    one_out, two_out = pack(me, basis, [one, two], parts)
    one_out = exchanged(one_out, "vecs")
    down = from_behind(lists, "rows", 1)
    matrix = spread_coefficients(me, coefficients, parts, ranks, vecs)
    z_ends = mix(matrix, ends_out, 0, ends.seg, vecs)
    z_ends = exchanged(z_ends, "vecs")
    two_out = exchanged(two_out, "vecs")
    hots = one_hots(min(ends.seg, 256), down, lower_cells, upper_cells, wide_count[:, :1])
    one_out[0], two_out[0] = kept(one_out[0]), kept(two_out[0])
    z_one = mix(matrix, one_out, 0, one.seg, vecs)
    z_one = exchanged(z_one, "vecs")
    plane_low, plane_high = end_planes(me, z_ends)
    from_below = from_behind(plane_high, "rows", 1)
    from_above = from_behind(plane_low, "rows", -1)
    link = link_terms(from_below, from_above, hots)
    z_two = mix(matrix, two_out, 0, two.seg, vecs)
    z_two = exchanged(z_two, "vecs")
    diagonals = [a.reshape(rows_local // LANES, LANES) for a in (stiffness, damping, mass)]
    eig = eigen_values[None, :]
    split = middle - 1
    eigvecs, residuals, edge, sums = part_one(
        me, [ends, one], z_ends + z_one, link, eig, diagonals, vecs, rows_local, parts,
        split,
    )
    eigvecs, residuals, sums = part_two(
        me, two, z_two, edge, eig, diagonals, sums, eigvecs, residuals, parts, split,
        subdomains,
    )
    total = lax.all_to_all(sums, "rows", 0, 0, tiled=True).sum(axis=(0, 1))
    vector_sq, residual_sq = total[:vecs], total[NP : NP + vecs]
    relative_norms = jnp.sqrt(residual_sq) / jnp.sqrt(vector_sq + 1.0)
    return (eigvecs, residuals, relative_norms)


def solution(mesh):
    placed = (
        P("vecs", "rows"),
        P(),
        P("vecs"),
        P("rows"),
        P("rows"),
        P("rows"),
        P("rows"),
        P("rows", None),
        P("rows", None),
    )
    return jax.shard_map(
        on_device,
        mesh=mesh,
        in_specs=placed,
        out_specs=(P("vecs", "rows"), P("vecs", "rows"), P("vecs")),
        check_vma=False,
    )
```

```python
import functools

import jax
import jax.numpy as jnp
from jax import lax
from jax.experimental import pallas as pl
from jax.experimental.pallas import tpu as pltpu
from jax.sharding import PartitionSpec as P


WID = 64
LANES = 128
SEGS = 8
NP = 16
BF = jnp.bfloat16
F32 = jnp.float32


def from_behind(value, axis, steps):
    count = lax.axis_size(axis)
    pairs = [(source, (source + steps) % count) for source in range(count)]
    return lax.ppermute(value, axis, pairs)


ANY = pl.BlockSpec(memory_space=pl.ANY)
VMEM = pl.BlockSpec(memory_space=pltpu.VMEM)
SMEM = pl.BlockSpec(memory_space=pltpu.SMEM)


def params(mib):
    return pltpu.CompilerParams(vmem_limit_bytes=mib * 1024 * 1024)


def cost(flops, nbytes):
    return pl.CostEstimate(flops=int(flops), bytes_accessed=int(nbytes), transcendentals=0)


class Chunk:
    def __init__(self, first, count, parts, planes):
        self.first = first or 0
        self.width = count * WID * WID // parts
        self.seg = self.width // SEGS
        self.jump = (planes - count) * WID * WID if first is None else 0
        self.parts = parts

    def start(self, v):
        base = self.first * WID * WID + v * self.width
        return base + jnp.where(2 * v >= self.parts, self.jump, 0) if self.jump else base


class Packing:
    def __init__(self, chunk, parts, me, basis_ref, outs, buf, laid, sem):
        self.chunk, self.buf, self.laid, self.reads = chunk, buf, laid, []
        self.turns = [*range(1, parts), 0]
        self.writes = [
            pltpu.make_async_copy(laid.at[k], outs[k], sem.at[1, k]) for k in range(parts)
        ]
        for k in range(parts):
            st = pl.multiple_of(chunk.start(lax.rem(me + k, parts)), LANES)
            self.reads.append(
                pltpu.make_async_copy(
                    basis_ref.at[:, pl.ds(st, chunk.width)], buf.at[k], sem.at[0, k]
                )
            )
        for k in self.turns:
            self.reads[k].start()

    def finish(self):
        ranks, seg = self.buf.shape[1], self.chunk.seg
        full = ranks // 8 * 8
        before = None
        for k in self.turns:
            self.reads[k].wait()
            tail = []
            for c in range(SEGS):
                cut = slice(c * seg, (c + 1) * seg)
                self.laid[k, c * full : (c + 1) * full, :] = self.buf[k, 0:full, cut]
                tail.append(self.buf[k, full:ranks, cut])
            self.laid[k, SEGS * full : SEGS * ranks, :] = jnp.concatenate(tail, axis=0)
            if before is not None:
                self.writes[before].start()
            before = k
        self.writes[before].start()

    def wait(self):
        for write in self.writes:
            write.wait()


def packed_shape(chunk, ranks):
    return jax.ShapeDtypeStruct((SEGS * ranks, chunk.seg), BF)


def pack_scratch(chunk, ranks, parts):
    return [
        pltpu.VMEM((parts, ranks, chunk.width), BF),
        pltpu.VMEM((parts, SEGS * ranks, chunk.seg), BF),
        pltpu.SemaphoreType.DMA((2, parts)),
    ]


def pack_kernel(chunks, parts, me_ref, basis_ref, *rest):
    n = parts * len(chunks)
    outs, scratch = rest[:n], rest[n:]
    work = [
        Packing(
            chunk, parts, me_ref[0], basis_ref, outs[i * parts : (i + 1) * parts],
            *scratch[3 * i : 3 * i + 3]
        )
        for i, chunk in enumerate(chunks)
    ]
    for w in work:
        w.finish()
    for w in work:
        w.wait()


def pack(me, basis, chunks, parts):
    ranks = basis.shape[0]
    shapes, scratch = [], []
    for chunk in chunks:
        shapes += [packed_shape(chunk, ranks)] * parts
        scratch += pack_scratch(chunk, ranks, parts)
    packed = pl.pallas_call(
        functools.partial(pack_kernel, chunks, parts),
        out_shape=shapes,
        in_specs=[SMEM, ANY],
        out_specs=[ANY] * len(shapes),
        scratch_shapes=scratch,
        compiler_params=params(60),
        cost_estimate=cost(1, 4 * parts * ranks * sum(chunk.width for chunk in chunks)),
        name="pack",
    )(me, basis)
    return [list(packed[i * parts : (i + 1) * parts]) for i in range(len(chunks))]


def orders(shape, axis, main, rest):
    i = lax.broadcasted_iota(jnp.int32, shape, axis)
    body, tail = i < main * SEGS, i - main * SEGS
    entry = jnp.where(body, lax.rem(i, main), main + lax.rem(tail, rest))
    return entry, jnp.where(body, lax.div(i, main), lax.div(tail, rest))


def spread(parts, me, coef_ref, out_ref):
    wide, total = coef_ref.shape
    ranks, vecs = total // parts, wide // parts
    rows, cols = out_ref.shape[1] // parts, out_ref.shape[2]
    full, vfull = ranks // 8 * 8, vecs // 8 * 8
    col_rank, col_seg = orders((1, cols), 1, full, ranks - full)
    row_vec, row_seg = orders((rows, 1), 0, vfull, vecs - vfull)
    coef = coef_ref[...]
    same = row_seg == col_seg
    for k in range(parts):
        source = lax.rem(me - k + parts, parts) * ranks
        pick = lax.broadcasted_iota(jnp.int32, (total, cols), 0) == col_rank + source
        by_col = jnp.dot(
            coef, jnp.where(pick, 1.0, 0.0).astype(BF), preferred_element_type=F32
        ).astype(BF)
        for o in range(parts):
            owner = lax.rem(me + o, parts) * vecs
            pick = lax.broadcasted_iota(jnp.int32, (rows, wide), 1) == row_vec + owner
            block = jnp.dot(
                jnp.where(pick, 1.0, 0.0).astype(BF), by_col, preferred_element_type=F32
            )
            out_ref[k, o * rows : (o + 1) * rows, :] = jnp.where(same, block, 0.0).astype(BF)


def spread_coefficients(me, coefficients, parts, ranks, vecs):
    nc, nr = SEGS * ranks, SEGS * vecs
    return pl.pallas_call(
        lambda me_ref, coef_ref, out_ref: spread(parts, me_ref[0], coef_ref, out_ref),
        out_shape=jax.ShapeDtypeStruct((parts, parts * nr, nc), BF),
        in_specs=[SMEM, VMEM],
        out_specs=VMEM,
        compiler_params=params(8),
        cost_estimate=cost(20 * parts * parts * nr * nc, 2 * parts * parts * nr * nc),
        name="spread",
    )(me, coefficients.T)


def mix_kernel(parts, lane, seg, l_ref, *rest):
    ys, outs = rest[:parts], rest[parts:]
    rows = outs[0].shape[0]
    step = 256

    def body(at, step):
        total = None
        for k in range(parts):
            part = jnp.dot(
                l_ref[k], ys[k][:, pl.ds(lane + at, step)], preferred_element_type=F32
            )
            total = part if total is None else total + part
        for o in range(parts):
            outs[o][:, pl.ds(at, step)] = total[o * rows : (o + 1) * rows].astype(BF)

    @pl.loop(0, seg // step)
    def _(i):
        body(pl.multiple_of(i * step, step), step)

    if seg % step:
        body(seg // step * step, seg % step)


def mix(matrix, packed, lane, seg, vecs):
    parts, rows, depth = matrix.shape
    return pl.pallas_call(
        functools.partial(mix_kernel, parts, lane, seg),
        out_shape=[jax.ShapeDtypeStruct((SEGS * vecs, seg), BF)] * parts,
        in_specs=[VMEM] * (1 + parts),
        out_specs=[VMEM] * parts,
        compiler_params=params(12),
        cost_estimate=cost(2 * rows * parts * depth * seg, 2 * (rows + parts * depth) * seg),
        name="mix",
    )(matrix, *packed)


def one_hot_kernel(low, down_ref, lower_ref, upper_ref, count_ref, g_ref, s_ref, seg_ref):
    slots = lower_ref.shape[1]
    shift = low.bit_length() - 1
    step = 256
    centred = lambda cells: (jnp.bitwise_and(cells, low - 1) - low // 2).astype(F32).astype(BF)
    lane = centred(lax.broadcasted_iota(jnp.int32, (low, step), 0))
    across = centred(lax.broadcasted_iota(jnp.int32, (LANES, low), 1))
    one, none = jnp.ones((), BF), jnp.zeros((), BF)
    ways = (
        (down_ref, 0, down_ref, slots, down_ref[:, 2 * slots : 2 * slots + 1]),
        (upper_ref, 0, lower_ref, 0, count_ref[...]),
    )

    @pl.loop(0, slots // step)
    def _(i):
        at = pl.ds(pl.multiple_of(i * step, step), step)
        slot = lax.broadcasted_iota(jnp.int32, (1, step), 1) + i * step
        for d, (from_ref, f0, to_ref, t0, count) in enumerate(ways):
            g = from_ref[:, pl.ds(pl.multiple_of(f0 + i * step, step), step)]
            s = to_ref[:, pl.ds(pl.multiple_of(t0 + i * step, step), step)]
            wanted = jnp.broadcast_to(centred(g), (low, step))
            g_ref[d, :, at] = jnp.where(lane == wanted, one, none)
            s_low = (jnp.bitwise_and(s, low - 1) - low // 2).astype(F32)
            for j in range(0, step, LANES):
                turned = jnp.broadcast_to(s_low[:, j : j + LANES], (LANES, LANES)).T.astype(BF)
                turned = jnp.concatenate([turned] * (low // LANES), axis=1)
                rows = pl.ds(pl.multiple_of(i * step + j, LANES), LANES)
                s_ref[d, rows, :] = jnp.where(turned == across, one, none)
            seg_ref[2 * d : 2 * d + 1, at] = lax.shift_right_logical(g, shift)
            seg_ref[2 * d + 1 : 2 * d + 2, at] = jnp.where(
                slot < count, lax.shift_right_logical(s, shift), -1
            )


def one_hots(low, down, lower, upper, count):
    slots = lower.shape[1]
    hot = jax.ShapeDtypeStruct((2, low, slots), BF)
    hot_down = jax.ShapeDtypeStruct((2, slots, low), BF)
    return pl.pallas_call(
        functools.partial(one_hot_kernel, low),
        out_shape=(hot, hot_down, jax.ShapeDtypeStruct((4, slots), jnp.int32)),
        in_specs=[VMEM] * 4,
        out_specs=[VMEM] * 3,
        compiler_params=params(20),
        cost_estimate=cost(40 * low * slots, 8 * low * slots),
        name="one_hots",
    )(down, lower, upper, count)


def link_kernel(below_ref, above_ref, g_ref, s_ref, seg_ref, out_ref, put):
    rows, wide = below_ref.shape
    low, slots = g_ref.shape[1:]
    per = wide // low
    vfull = 8
    vrest = rows // SEGS - vfull
    step = 512
    tail_rows = SEGS * vrest
    tail_seg = lax.broadcasted_iota(jnp.int32, (tail_rows, 1), 0) // vrest
    planes = [
        jnp.concatenate([ref[:, h * low : (h + 1) * low] for h in range(per)], axis=0)
        for ref in (below_ref, above_ref)
    ]
    for i in range(slots // step):
        at = slice(i * step, (i + 1) * step)
        for d, plane in enumerate(planes):
            got = jnp.dot(plane, g_ref[d, :, at], preferred_element_type=F32)
            gh, sh = seg_ref[2 * d : 2 * d + 1, at], seg_ref[2 * d + 1 : 2 * d + 2, at]
            main, tail = got[0:vfull], jnp.zeros((tail_rows, step), F32)
            for h in range(per):
                for c in range(SEGS):
                    part = got[h * rows + c * vfull : h * rows + (c + 1) * vfull]
                    main = jnp.where(gh == c * per + h, part, main)
                part = got[h * rows + SEGS * vfull : (h + 1) * rows]
                tail = jnp.where(gh == tail_seg * per + h, part, tail)
            shift = vrest
            while shift < tail_rows:
                tail = tail + pltpu.roll(tail, shift, 0)
                shift *= 2
            pieces = []
            for h in range(per):
                pieces += [jnp.where(sh == c * per + h, main, 0.0) for c in range(SEGS)]
                pieces.append(jnp.where(sh == tail_seg * per + h, tail, 0.0))
            put[d, :, at] = jnp.concatenate(pieces, axis=0).astype(BF)

    for d in range(2):
        total = jnp.dot(put[d], s_ref[d], preferred_element_type=F32)
        for h in range(per):
            for c in range(SEGS):
                for k in range(low // LANES):
                    t = d * 32 + (c * per + h) * (low // LANES) + k
                    at = slice(k * LANES, (k + 1) * LANES)
                    first = h * rows + c * 8
                    out_ref[t, 0:8, :] = total[first : first + 8, at]
                    first = h * rows + SEGS * 8 + c * vrest
                    out_ref[t, 8 : 8 + vrest, :] = total[first : first + vrest, at]


def link_terms(below, above, hots):
    rows = below.size // hots[0].shape[1]
    low, slots = hots[0].shape[1:]
    return pl.pallas_call(
        link_kernel,
        out_shape=jax.ShapeDtypeStruct((64, NP, LANES), F32),
        in_specs=[VMEM] * 5,
        out_specs=VMEM,
        scratch_shapes=[pltpu.VMEM((2, rows, slots), BF)],
        compiler_params=params(10),
        cost_estimate=cost(8 * rows * low * slots, 8 * rows * low),
        name="links",
    )(below, above, *hots)


def ends_kernel(parts, me_ref, *rest):
    z_refs, (low_ref, high_ref) = rest[:parts], rest[parts:]
    for k in range(parts):
        v = lax.rem(me_ref[0] - k + parts, parts)

        @pl.when(v == 0)
        def _():
            low_ref[...] = z_refs[k][...]

        @pl.when(v == parts - 1)
        def _():
            high_ref[...] = z_refs[k][...]


def end_planes(me, zs):
    parts = len(zs)
    shape = jax.ShapeDtypeStruct(zs[0].shape, BF)
    return pl.pallas_call(
        functools.partial(ends_kernel, parts),
        out_shape=(shape, shape),
        in_specs=[SMEM] + [VMEM] * parts,
        out_specs=(VMEM, VMEM),
        compiler_params=params(8),
        cost_estimate=cost(1, 8 * zs[0].size * parts),
        name="ends",
    )(me, *zs)


def unpack(cells, tile0, chunk, me, parts, z_refs, vrest):
    for k in range(parts):
        first = chunk.start(lax.rem(me - k + parts, parts)) // LANES - tile0
        per = chunk.seg // LANES
        for c in range(SEGS):
            for i in range(per):
                at = slice(i * LANES, (i + 1) * LANES)
                t = first + c * per + i
                low = SEGS * 8 + c * vrest
                cells[t, 0:8, :] = z_refs[k][c * 8 : (c + 1) * 8, at].astype(F32)
                cells[t, 8 : 8 + vrest, :] = z_refs[k][low : low + vrest, at].astype(F32)


class Output:
    def __init__(self, refs, bufs, sem, shifts):
        self.refs, self.bufs, self.sem, self.shifts = refs, bufs, sem, shifts
        self.copies = []

    def send(self, first, last):
        lanes = (last - first) * WID * WID
        to = pl.ds(first * WID * WID, lanes)
        shift = self.shifts.get(first, self.shifts.get(None, 0))
        at = pl.ds((first - shift) * WID * WID, lanes)
        for i in range(2):
            copy = pltpu.make_async_copy(
                self.bufs[i].at[:, at], self.refs[i].at[:, to], self.sem.at[len(self.copies)]
            )
            copy.start()
            self.copies.append(copy)

    def wait(self):
        for copy in self.copies:
            copy.wait()


def cuts(low, high, step):
    marks = list(range(low, high, step))
    return list(zip(marks, marks[1:] + [high]))


class Terms:
    def __init__(self, eig_ref, stiff_ref, damp_ref, mass_ref):
        vecs = eig_ref.shape[1]
        sub = lax.broadcasted_iota(jnp.int32, (NP, vecs), 0)
        own = sub == lax.broadcasted_iota(jnp.int32, (NP, vecs), 1)
        eig = jnp.sum(jnp.where(own, eig_ref[...], 0.0), axis=1, keepdims=True)
        self.eig = jnp.broadcast_to(eig, (NP, LANES))
        self.eig_sq = self.eig * self.eig
        self.coupling = self.eig_sq * 0.1 + self.eig * 0.3 + 1.0
        self.diagonals = (stiff_ref, damp_ref, mass_ref)
        lane = lax.broadcasted_iota(jnp.int32, (1, LANES), 1)
        self.low_half = lane < WID
        column = jnp.bitwise_and(lane, WID - 1)
        self.not_first, self.not_last = column > 0, column < WID - 1


def one_plane(terms, cells, z, z0, carry, link, outs):
    tiles = WID * WID // LANES
    vsum, rsum = carry
    base = (z - z0) * tiles
    stiff_ref, damp_ref, mass_ref = terms.diagonals
    for i in range(tiles):
        x = cells[base + i]
        ahead = cells[base + i + 1] if i + 1 < tiles else None
        behind = cells[base + i - 1] if i > 0 else None
        if behind is None:
            across = jnp.where(terms.low_half, ahead, 0.0)
        elif ahead is None:
            across = jnp.where(terms.low_half, 0.0, behind)
        else:
            across = jnp.where(terms.low_half, ahead, behind)
        total = pltpu.roll(x + across, WID, 1)
        total = total + jnp.where(terms.not_first, pltpu.roll(x, 1, 1), 0.0)
        total = total + jnp.where(terms.not_last, pltpu.roll(x, LANES - 1, 1), 0.0)
        if link is None:
            total = total + (cells[base + i - tiles] + cells[base + i + tiles])
        else:
            link_ref, offset, side = link
            total = total + (link_ref[offset + i] + cells[base + i + side * tiles])
        row = pl.ds(z * tiles + i, 1)
        diagonal = (
            terms.eig_sq * mass_ref[row, :] + terms.eig * damp_ref[row, :] + stiff_ref[row, :]
        )
        res = diagonal * x - terms.coupling * total
        if outs is not None:
            vec_ref, res_ref, o0 = outs
            vecs = vec_ref.shape[0]
            at = pl.ds(pl.multiple_of(z * WID * WID - o0 + i * LANES, LANES), LANES)
            vec_ref[:, at] = x[:vecs].astype(BF)
            res_ref[:, at] = res[:vecs].astype(BF)
        vsum = vsum + x * x
        rsum = rsum + res * res
    return vsum, rsum


def finished_planes(terms, cells, z0, carry, links, outs, out, low, high, ends, step):
    ready = []
    for z in ends:
        carry = one_plane(terms, cells, z, z0, carry, links.get(z), outs(z))
        ready.append((z, z + 1))
    for first, end in cuts(low, high, step):
        carry = lax.fori_loop(
            first, end, lambda z, c: one_plane(terms, cells, z, z0, c, None, outs(first)), carry
        )
        for cut in ready:
            out.send(*cut)
        ready = [(first, end)]
    return carry, ready


def part_one_kernel(chunks, parts, planes, split, me_ref, *rest):
    nz = parts * len(chunks)
    z_refs, rest = rest[:nz], rest[nz:]
    link_ref, eig_ref, stiff_ref, damp_ref, mass_ref = rest[:5]
    vec_ref, res_ref, edge_ref, sum_ref, cells, vec_buf, res_buf, sem = rest[5:]
    vecs = vec_ref.shape[0]
    tiles = WID * WID // LANES
    for i, chunk in enumerate(chunks):
        unpack(cells, 0, chunk, me_ref[0], parts, z_refs[i * parts : (i + 1) * parts], vecs - 8)
    terms = Terms(eig_ref, stiff_ref, damp_ref, mass_ref)
    moved = (planes - 1 - split) * WID * WID
    outs = lambda z: (vec_buf, res_buf, moved if z == planes - 1 else 0)
    out = Output((vec_ref, res_ref), (vec_buf, res_buf), sem, {planes - 1: planes - 1 - split})
    zero = jnp.zeros((NP, LANES), F32)
    links = {0: (link_ref, 0, 1), planes - 1: (link_ref, tiles, -1)}
    carry, ready = finished_planes(
        terms, cells, 0, (zero, zero), links, outs, out, 1, split, (0, planes - 1), 3
    )
    edge_ref[0 : 2 * tiles] = cells[(split - 1) * tiles : (split + 1) * tiles]
    edge_ref[2 * tiles : 4 * tiles] = cells[(planes - 2) * tiles : planes * tiles]
    sum_ref[0], sum_ref[1] = carry
    for cut in ready:
        out.send(*cut)
    out.wait()


def part_two_kernel(chunk, parts, planes, split, me_ref, *rest):
    z_refs, rest = rest[:parts], rest[parts:]
    edge_ref, eig_ref, stiff_ref, damp_ref, mass_ref, early_ref, _, _ = rest[:8]
    vec_ref, res_ref, out_ref, cells, vec_buf, res_buf, sem = rest[8:]
    vecs = vec_ref.shape[0]
    tiles = WID * WID // LANES
    z0 = split - 1
    cells[0 : 2 * tiles] = edge_ref[0 : 2 * tiles]
    cells[(planes - 2 - z0) * tiles : (planes - z0) * tiles] = edge_ref[2 * tiles : 4 * tiles]
    unpack(cells, z0 * tiles, chunk, me_ref[0], parts, z_refs, vecs - 8)
    terms = Terms(eig_ref, stiff_ref, damp_ref, mass_ref)
    outs = lambda z: (vec_buf, res_buf, split * WID * WID)
    out = Output((vec_ref, res_ref), (vec_buf, res_buf), sem, {None: split})
    carry = (early_ref[0], early_ref[1])
    carry, ready = finished_planes(terms, cells, z0, carry, {}, outs, out, split, planes - 1, (), 1)
    vsum, rsum = carry
    vrow = jnp.broadcast_to(jnp.sum(vsum, axis=1, keepdims=True), (NP, LANES))
    rrow = jnp.broadcast_to(jnp.sum(rsum, axis=1, keepdims=True), (NP, LANES))
    sub = lax.broadcasted_iota(jnp.int32, (NP, LANES), 0)
    wide = lax.broadcasted_iota(jnp.int32, (NP, LANES), 1)
    both = jnp.where((sub == wide) & (sub < vecs), vrow, 0.0)
    both = both + jnp.where((sub + NP == wide) & (sub < vecs), rrow, 0.0)
    line = jnp.sum(both, axis=0, keepdims=True)
    out_ref[...] = jnp.broadcast_to(line[None], out_ref.shape)
    for cut in ready:
        out.send(*cut)
    out.wait()


def buffers(planes, kept_planes, vecs):
    tiles = WID * WID // LANES
    return [
        pltpu.VMEM((planes * tiles, NP, LANES), F32),
        pltpu.VMEM((vecs, kept_planes * WID * WID), BF),
        pltpu.VMEM((vecs, kept_planes * WID * WID), BF),
        pltpu.SemaphoreType.DMA((16,)),
    ]


def part_one(me, chunks, zs, link, eig, diagonals, vecs, rows_local, parts, split):
    planes = rows_local // (WID * WID)
    tiles = WID * WID // LANES
    whole = jax.ShapeDtypeStruct((vecs, rows_local), BF)
    return pl.pallas_call(
        functools.partial(part_one_kernel, chunks, parts, planes, split),
        out_shape=(
            whole,
            whole,
            jax.ShapeDtypeStruct((4 * tiles, NP, LANES), F32),
            jax.ShapeDtypeStruct((2, NP, LANES), F32),
        ),
        in_specs=[SMEM] + [VMEM] * (len(zs) + 5),
        out_specs=(ANY, ANY, VMEM, VMEM),
        scratch_shapes=buffers(planes, split + 1, vecs),
        compiler_params=params(20),
        cost_estimate=cost(2000 * NP * rows_local, 4 * NP * rows_local),
        name="part_one",
    )(me, *zs, link, eig, *diagonals)


def part_two(me, chunk, zs, edge, eig, diagonals, early, vec, res, parts, split, copies):
    vecs, rows_local = vec.shape
    planes = rows_local // (WID * WID)
    whole = jax.ShapeDtypeStruct((vecs, rows_local), BF)
    first = 1 + parts + 6
    return pl.pallas_call(
        functools.partial(part_two_kernel, chunk, parts, planes, split),
        out_shape=(whole, whole, jax.ShapeDtypeStruct((copies, 1, LANES), F32)),
        in_specs=[SMEM] + [VMEM] * (parts + 6) + [ANY, ANY],
        out_specs=(ANY, ANY, VMEM),
        scratch_shapes=buffers(planes - split + 1, planes - 1 - split, vecs),
        input_output_aliases={first: 0, first + 1: 1},
        compiler_params=params(20),
        cost_estimate=cost(2000 * NP * rows_local, 4 * NP * rows_local),
        name="part_two",
    )(me, *zs, edge, eig, *diagonals, early, vec, res)


def kept(value):
    def kernel(from_ref, to_ref):
        to_ref[...] = from_ref[...]

    return pl.pallas_call(
        kernel,
        out_shape=jax.ShapeDtypeStruct(value.shape, value.dtype),
        in_specs=[VMEM],
        out_specs=VMEM,
        compiler_params=params(4),
        cost_estimate=cost(1, 4 * value.size),
        name="kept",
    )(value)


def exchanged(arrays, axis):
    return [arrays[0]] + [from_behind(arrays[k], axis, k) for k in range(1, len(arrays))]


def on_device(
    basis,
    coefficients,
    eigen_values,
    stiffness,
    damping,
    mass,
    link_count,
    lower_cells,
    upper_cells,
):
    parts = lax.axis_size("vecs")
    subdomains = lax.axis_size("rows")
    vecs = eigen_values.shape[0]
    ranks, rows_local = basis.shape
    planes = rows_local // (WID * WID)
    me = lax.axis_index("vecs").astype(jnp.int32)[None]
    ends = Chunk(None, 4, parts, planes)
    middle = (planes - 4) // 2 + 2
    one = Chunk(2, middle - 2, parts, planes)
    two = Chunk(middle, planes - 2 - middle, parts, planes)
    wide_count = jnp.broadcast_to(link_count[:, None], (1, LANES))
    lists = jnp.concatenate([lower_cells, upper_cells, wide_count], axis=1)
    (ends_out,) = pack(me, basis, [ends], parts)
    ends_out = exchanged(ends_out, "vecs")
    one_out, two_out = pack(me, basis, [one, two], parts)
    one_out = exchanged(one_out, "vecs")
    down = from_behind(lists, "rows", 1)
    matrix = spread_coefficients(me, coefficients, parts, ranks, vecs)
    z_ends = mix(matrix, ends_out, 0, ends.seg, vecs)
    z_ends = exchanged(z_ends, "vecs")
    two_out = exchanged(two_out, "vecs")
    hots = one_hots(min(ends.seg, 256), down, lower_cells, upper_cells, wide_count[:, :1])
    one_out[0], two_out[0] = kept(one_out[0]), kept(two_out[0])
    z_one = mix(matrix, one_out, 0, one.seg, vecs)
    z_one = exchanged(z_one, "vecs")
    plane_low, plane_high = end_planes(me, z_ends)
    from_below = from_behind(plane_high, "rows", 1)
    from_above = from_behind(plane_low, "rows", -1)
    link = link_terms(from_below, from_above, hots)
    z_two = mix(matrix, two_out, 0, two.seg, vecs)
    z_two = exchanged(z_two, "vecs")
    diagonals = [a.reshape(rows_local // LANES, LANES) for a in (stiffness, damping, mass)]
    eig = eigen_values[None, :]
    split = middle - 1
    eigvecs, residuals, edge, sums = part_one(
        me, [ends, one], z_ends + z_one, link, eig, diagonals, vecs, rows_local, parts,
        split,
    )
    eigvecs, residuals, sums = part_two(
        me, two, z_two, edge, eig, diagonals, sums, eigvecs, residuals, parts, split,
        subdomains,
    )
    total = lax.all_to_all(sums, "rows", 0, 0, tiled=True).sum(axis=(0, 1))
    vector_sq, residual_sq = total[:vecs], total[NP : NP + vecs]
    relative_norms = jnp.sqrt(residual_sq) / jnp.sqrt(vector_sq + 1.0)
    return (eigvecs, residuals, relative_norms)


def solution(mesh):
    placed = (
        P("vecs", "rows"),
        P(),
        P("vecs"),
        P("rows"),
        P("rows"),
        P("rows"),
        P("rows"),
        P("rows", None),
        P("rows", None),
    )
    return jax.shard_map(
        on_device,
        mesh=mesh,
        in_specs=placed,
        out_specs=(P("vecs", "rows"), P("vecs", "rows"), P("vecs")),
        check_vma=False,
    )
```

```python
import functools

import jax
import jax.numpy as jnp
from jax import lax
from jax.experimental import pallas as pl
from jax.experimental.pallas import tpu as pltpu
from jax.sharding import PartitionSpec as P


WID = 64
LANES = 128
SEGS = 8
NP = 16
BF = jnp.bfloat16
F32 = jnp.float32


def from_behind(value, axis, steps):
    count = lax.axis_size(axis)
    pairs = [(source, (source + steps) % count) for source in range(count)]
    return lax.ppermute(value, axis, pairs)


ANY = pl.BlockSpec(memory_space=pl.ANY)
VMEM = pl.BlockSpec(memory_space=pltpu.VMEM)
SMEM = pl.BlockSpec(memory_space=pltpu.SMEM)


def params(mib):
    return pltpu.CompilerParams(vmem_limit_bytes=mib * 1024 * 1024)


def cost(flops, nbytes):
    return pl.CostEstimate(flops=int(flops), bytes_accessed=int(nbytes), transcendentals=0)


class Chunk:
    def __init__(self, first, count, parts, planes):
        self.first = first or 0
        self.width = count * WID * WID // parts
        self.seg = self.width // SEGS
        self.jump = (planes - count) * WID * WID if first is None else 0
        self.parts = parts

    def start(self, v):
        base = self.first * WID * WID + v * self.width
        return base + jnp.where(2 * v >= self.parts, self.jump, 0) if self.jump else base


class Packing:
    def __init__(self, chunk, parts, me, basis_ref, outs, buf, laid, sem):
        self.chunk, self.buf, self.laid, self.reads = chunk, buf, laid, []
        self.turns = [*range(1, parts), 0]
        self.writes = [
            pltpu.make_async_copy(laid.at[k], outs[k], sem.at[1, k]) for k in range(parts)
        ]
        for k in range(parts):
            st = pl.multiple_of(chunk.start(lax.rem(me + k, parts)), LANES)
            self.reads.append(
                pltpu.make_async_copy(
                    basis_ref.at[:, pl.ds(st, chunk.width)], buf.at[k], sem.at[0, k]
                )
            )
        for k in self.turns:
            self.reads[k].start()

    def finish(self):
        ranks, seg = self.buf.shape[1], self.chunk.seg
        full = ranks // 8 * 8
        before = None
        for k in self.turns:
            self.reads[k].wait()
            tail = []
            for c in range(SEGS):
                cut = slice(c * seg, (c + 1) * seg)
                self.laid[k, c * full : (c + 1) * full, :] = self.buf[k, 0:full, cut]
                tail.append(self.buf[k, full:ranks, cut])
            self.laid[k, SEGS * full : SEGS * ranks, :] = jnp.concatenate(tail, axis=0)
            if before is not None:
                self.writes[before].start()
            before = k
        self.writes[before].start()

    def wait(self):
        for write in self.writes:
            write.wait()


def packed_shape(chunk, ranks):
    return jax.ShapeDtypeStruct((SEGS * ranks, chunk.seg), BF)


def pack_scratch(chunk, ranks, parts):
    return [
        pltpu.VMEM((parts, ranks, chunk.width), BF),
        pltpu.VMEM((parts, SEGS * ranks, chunk.seg), BF),
        pltpu.SemaphoreType.DMA((2, parts)),
    ]


def pack_kernel(chunks, parts, me_ref, basis_ref, *rest):
    n = parts * len(chunks)
    outs, scratch = rest[:n], rest[n:]
    work = [
        Packing(
            chunk, parts, me_ref[0], basis_ref, outs[i * parts : (i + 1) * parts],
            *scratch[3 * i : 3 * i + 3]
        )
        for i, chunk in enumerate(chunks)
    ]
    for w in work:
        w.finish()
    for w in work:
        w.wait()


def pack(me, basis, chunks, parts):
    ranks = basis.shape[0]
    shapes, scratch = [], []
    for chunk in chunks:
        shapes += [packed_shape(chunk, ranks)] * parts
        scratch += pack_scratch(chunk, ranks, parts)
    packed = pl.pallas_call(
        functools.partial(pack_kernel, chunks, parts),
        out_shape=shapes,
        in_specs=[SMEM, ANY],
        out_specs=[ANY] * len(shapes),
        scratch_shapes=scratch,
        compiler_params=params(60),
        cost_estimate=cost(1, 4 * parts * ranks * sum(chunk.width for chunk in chunks)),
        name="pack",
    )(me, basis)
    return [list(packed[i * parts : (i + 1) * parts]) for i in range(len(chunks))]


def orders(shape, axis, main, rest):
    i = lax.broadcasted_iota(jnp.int32, shape, axis)
    body, tail = i < main * SEGS, i - main * SEGS
    entry = jnp.where(body, lax.rem(i, main), main + lax.rem(tail, rest))
    return entry, jnp.where(body, lax.div(i, main), lax.div(tail, rest))


def spread(parts, me, coef_ref, out_ref):
    wide, total = coef_ref.shape
    ranks, vecs = total // parts, wide // parts
    rows, cols = out_ref.shape[1] // parts, out_ref.shape[2]
    full, vfull = ranks // 8 * 8, vecs // 8 * 8
    col_rank, col_seg = orders((1, cols), 1, full, ranks - full)
    row_vec, row_seg = orders((rows, 1), 0, vfull, vecs - vfull)
    coef = coef_ref[...]
    same = row_seg == col_seg
    for k in range(parts):
        source = lax.rem(me - k + parts, parts) * ranks
        pick = lax.broadcasted_iota(jnp.int32, (total, cols), 0) == col_rank + source
        by_col = jnp.dot(
            coef, jnp.where(pick, 1.0, 0.0).astype(BF), preferred_element_type=F32
        ).astype(BF)
        for o in range(parts):
            owner = lax.rem(me + o, parts) * vecs
            pick = lax.broadcasted_iota(jnp.int32, (rows, wide), 1) == row_vec + owner
            block = jnp.dot(
                jnp.where(pick, 1.0, 0.0).astype(BF), by_col, preferred_element_type=F32
            )
            out_ref[k, o * rows : (o + 1) * rows, :] = jnp.where(same, block, 0.0).astype(BF)


def spread_coefficients(me, coefficients, parts, ranks, vecs):
    nc, nr = SEGS * ranks, SEGS * vecs
    return pl.pallas_call(
        lambda me_ref, coef_ref, out_ref: spread(parts, me_ref[0], coef_ref, out_ref),
        out_shape=jax.ShapeDtypeStruct((parts, parts * nr, nc), BF),
        in_specs=[SMEM, VMEM],
        out_specs=VMEM,
        compiler_params=params(8),
        cost_estimate=cost(20 * parts * parts * nr * nc, 2 * parts * parts * nr * nc),
        name="spread",
    )(me, coefficients.T)


def mix_kernel(parts, lane, seg, l_ref, *rest):
    ys, outs = rest[:parts], rest[parts:]
    rows = outs[0].shape[0]
    step = 256

    def body(at, step):
        total = None
        for k in range(parts):
            part = jnp.dot(
                l_ref[k], ys[k][:, pl.ds(lane + at, step)], preferred_element_type=F32
            )
            total = part if total is None else total + part
        for o in range(parts):
            outs[o][:, pl.ds(at, step)] = total[o * rows : (o + 1) * rows].astype(BF)

    @pl.loop(0, seg // step)
    def _(i):
        body(pl.multiple_of(i * step, step), step)

    if seg % step:
        body(seg // step * step, seg % step)


def mix(matrix, packed, lane, seg, vecs):
    parts, rows, depth = matrix.shape
    return pl.pallas_call(
        functools.partial(mix_kernel, parts, lane, seg),
        out_shape=[jax.ShapeDtypeStruct((SEGS * vecs, seg), BF)] * parts,
        in_specs=[VMEM] * (1 + parts),
        out_specs=[VMEM] * parts,
        compiler_params=params(12),
        cost_estimate=cost(2 * rows * parts * depth * seg, 2 * (rows + parts * depth) * seg),
        name="mix",
    )(matrix, *packed)


def one_hot_kernel(low, down_ref, lower_ref, upper_ref, count_ref, g_ref, s_ref, seg_ref):
    slots = lower_ref.shape[1]
    shift = low.bit_length() - 1
    step = 256
    centred = lambda cells: (jnp.bitwise_and(cells, low - 1) - low // 2).astype(F32).astype(BF)
    lane = centred(lax.broadcasted_iota(jnp.int32, (low, step), 0))
    across = centred(lax.broadcasted_iota(jnp.int32, (LANES, low), 1))
    one, none = jnp.ones((), BF), jnp.zeros((), BF)
    ways = (
        (down_ref, 0, down_ref, slots, down_ref[:, 2 * slots : 2 * slots + 1]),
        (upper_ref, 0, lower_ref, 0, count_ref[...]),
    )

    @pl.loop(0, slots // step)
    def _(i):
        at = pl.ds(pl.multiple_of(i * step, step), step)
        slot = lax.broadcasted_iota(jnp.int32, (1, step), 1) + i * step
        for d, (from_ref, f0, to_ref, t0, count) in enumerate(ways):
            g = from_ref[:, pl.ds(pl.multiple_of(f0 + i * step, step), step)]
            s = to_ref[:, pl.ds(pl.multiple_of(t0 + i * step, step), step)]
            wanted = jnp.broadcast_to(centred(g), (low, step))
            g_ref[d, :, at] = jnp.where(lane == wanted, one, none)
            s_low = (jnp.bitwise_and(s, low - 1) - low // 2).astype(F32)
            for j in range(0, step, LANES):
                turned = jnp.broadcast_to(s_low[:, j : j + LANES], (LANES, LANES)).T.astype(BF)
                turned = jnp.concatenate([turned] * (low // LANES), axis=1)
                rows = pl.ds(pl.multiple_of(i * step + j, LANES), LANES)
                s_ref[d, rows, :] = jnp.where(turned == across, one, none)
            seg_ref[2 * d : 2 * d + 1, at] = lax.shift_right_logical(g, shift)
            seg_ref[2 * d + 1 : 2 * d + 2, at] = jnp.where(
                slot < count, lax.shift_right_logical(s, shift), -1
            )


def one_hots(low, down, lower, upper, count):
    slots = lower.shape[1]
    hot = jax.ShapeDtypeStruct((2, low, slots), BF)
    hot_down = jax.ShapeDtypeStruct((2, slots, low), BF)
    return pl.pallas_call(
        functools.partial(one_hot_kernel, low),
        out_shape=(hot, hot_down, jax.ShapeDtypeStruct((4, slots), jnp.int32)),
        in_specs=[VMEM] * 4,
        out_specs=[VMEM] * 3,
        compiler_params=params(20),
        cost_estimate=cost(40 * low * slots, 8 * low * slots),
        name="one_hots",
    )(down, lower, upper, count)


def link_kernel(below_ref, above_ref, g_ref, s_ref, seg_ref, out_ref, put):
    rows, wide = below_ref.shape
    low, slots = g_ref.shape[1:]
    per = wide // low
    vfull = 8
    vrest = rows // SEGS - vfull
    step = 512
    tail_rows = SEGS * vrest
    tail_seg = lax.broadcasted_iota(jnp.int32, (tail_rows, 1), 0) // vrest
    planes = [
        jnp.concatenate([ref[:, h * low : (h + 1) * low] for h in range(per)], axis=0)
        for ref in (below_ref, above_ref)
    ]
    for i in range(slots // step):
        at = slice(i * step, (i + 1) * step)
        for d, plane in enumerate(planes):
            got = jnp.dot(plane, g_ref[d, :, at], preferred_element_type=F32)
            gh, sh = seg_ref[2 * d : 2 * d + 1, at], seg_ref[2 * d + 1 : 2 * d + 2, at]
            main, tail = got[0:vfull], jnp.zeros((tail_rows, step), F32)
            for h in range(per):
                for c in range(SEGS):
                    part = got[h * rows + c * vfull : h * rows + (c + 1) * vfull]
                    main = jnp.where(gh == c * per + h, part, main)
                part = got[h * rows + SEGS * vfull : (h + 1) * rows]
                tail = jnp.where(gh == tail_seg * per + h, part, tail)
            shift = vrest
            while shift < tail_rows:
                tail = tail + pltpu.roll(tail, shift, 0)
                shift *= 2
            pieces = []
            for h in range(per):
                pieces += [jnp.where(sh == c * per + h, main, 0.0) for c in range(SEGS)]
                pieces.append(jnp.where(sh == tail_seg * per + h, tail, 0.0))
            put[d, :, at] = jnp.concatenate(pieces, axis=0).astype(BF)

    for d in range(2):
        total = jnp.dot(put[d], s_ref[d], preferred_element_type=F32)
        for h in range(per):
            for c in range(SEGS):
                for k in range(low // LANES):
                    t = d * 32 + (c * per + h) * (low // LANES) + k
                    at = slice(k * LANES, (k + 1) * LANES)
                    first = h * rows + c * 8
                    out_ref[t, 0:8, :] = total[first : first + 8, at]
                    first = h * rows + SEGS * 8 + c * vrest
                    out_ref[t, 8 : 8 + vrest, :] = total[first : first + vrest, at]


def link_terms(below, above, hots):
    rows = below.size // hots[0].shape[1]
    low, slots = hots[0].shape[1:]
    return pl.pallas_call(
        link_kernel,
        out_shape=jax.ShapeDtypeStruct((64, NP, LANES), F32),
        in_specs=[VMEM] * 5,
        out_specs=VMEM,
        scratch_shapes=[pltpu.VMEM((2, rows, slots), BF)],
        compiler_params=params(10),
        cost_estimate=cost(8 * rows * low * slots, 8 * rows * low),
        name="links",
    )(below, above, *hots)


def ends_kernel(parts, me_ref, *rest):
    z_refs, (low_ref, high_ref) = rest[:parts], rest[parts:]
    for k in range(parts):
        v = lax.rem(me_ref[0] - k + parts, parts)

        @pl.when(v == 0)
        def _():
            low_ref[...] = z_refs[k][...]

        @pl.when(v == parts - 1)
        def _():
            high_ref[...] = z_refs[k][...]


def end_planes(me, zs):
    parts = len(zs)
    shape = jax.ShapeDtypeStruct(zs[0].shape, BF)
    return pl.pallas_call(
        functools.partial(ends_kernel, parts),
        out_shape=(shape, shape),
        in_specs=[SMEM] + [VMEM] * parts,
        out_specs=(VMEM, VMEM),
        compiler_params=params(8),
        cost_estimate=cost(1, 8 * zs[0].size * parts),
        name="ends",
    )(me, *zs)


def unpack(cells, tile0, chunk, me, parts, z_refs, vrest):
    for k in range(parts):
        first = chunk.start(lax.rem(me - k + parts, parts)) // LANES - tile0
        per = chunk.seg // LANES
        for c in range(SEGS):
            for i in range(per):
                at = slice(i * LANES, (i + 1) * LANES)
                t = first + c * per + i
                low = SEGS * 8 + c * vrest
                cells[t, 0:8, :] = z_refs[k][c * 8 : (c + 1) * 8, at].astype(F32)
                cells[t, 8 : 8 + vrest, :] = z_refs[k][low : low + vrest, at].astype(F32)


class Output:
    def __init__(self, refs, bufs, sem, shifts):
        self.refs, self.bufs, self.sem, self.shifts = refs, bufs, sem, shifts
        self.copies = []

    def send(self, first, last):
        lanes = (last - first) * WID * WID
        to = pl.ds(first * WID * WID, lanes)
        shift = self.shifts.get(first, self.shifts.get(None, 0))
        at = pl.ds((first - shift) * WID * WID, lanes)
        for i in range(2):
            copy = pltpu.make_async_copy(
                self.bufs[i].at[:, at], self.refs[i].at[:, to], self.sem.at[len(self.copies)]
            )
            copy.start()
            self.copies.append(copy)

    def wait(self):
        for copy in self.copies:
            copy.wait()


def cuts(low, high, step):
    marks = list(range(low, high, step))
    return list(zip(marks, marks[1:] + [high]))


class Terms:
    def __init__(self, eig_ref, stiff_ref, damp_ref, mass_ref):
        vecs = eig_ref.shape[1]
        sub = lax.broadcasted_iota(jnp.int32, (NP, vecs), 0)
        own = sub == lax.broadcasted_iota(jnp.int32, (NP, vecs), 1)
        eig = jnp.sum(jnp.where(own, eig_ref[...], 0.0), axis=1, keepdims=True)
        self.eig = jnp.broadcast_to(eig, (NP, LANES))
        self.eig_sq = self.eig * self.eig
        self.coupling = self.eig_sq * 0.1 + self.eig * 0.3 + 1.0
        self.diagonals = (stiff_ref, damp_ref, mass_ref)
        lane = lax.broadcasted_iota(jnp.int32, (1, LANES), 1)
        self.low_half = lane < WID
        column = jnp.bitwise_and(lane, WID - 1)
        self.not_first, self.not_last = column > 0, column < WID - 1


def one_plane(terms, cells, z, z0, carry, link, outs):
    tiles = WID * WID // LANES
    vsum, rsum = carry
    base = (z - z0) * tiles
    stiff_ref, damp_ref, mass_ref = terms.diagonals
    for i in range(tiles):
        x = cells[base + i]
        ahead = cells[base + i + 1] if i + 1 < tiles else None
        behind = cells[base + i - 1] if i > 0 else None
        if behind is None:
            across = jnp.where(terms.low_half, ahead, 0.0)
        elif ahead is None:
            across = jnp.where(terms.low_half, 0.0, behind)
        else:
            across = jnp.where(terms.low_half, ahead, behind)
        total = pltpu.roll(x + across, WID, 1)
        total = total + jnp.where(terms.not_first, pltpu.roll(x, 1, 1), 0.0)
        total = total + jnp.where(terms.not_last, pltpu.roll(x, LANES - 1, 1), 0.0)
        if link is None:
            total = total + (cells[base + i - tiles] + cells[base + i + tiles])
        else:
            link_ref, offset, side = link
            total = total + (link_ref[offset + i] + cells[base + i + side * tiles])
        row = pl.ds(z * tiles + i, 1)
        diagonal = (
            terms.eig_sq * mass_ref[row, :] + terms.eig * damp_ref[row, :] + stiff_ref[row, :]
        )
        res = diagonal * x - terms.coupling * total
        if outs is not None:
            vec_ref, res_ref, o0 = outs
            vecs = vec_ref.shape[0]
            at = pl.ds(pl.multiple_of(z * WID * WID - o0 + i * LANES, LANES), LANES)
            vec_ref[:, at] = x[:vecs].astype(BF)
            res_ref[:, at] = res[:vecs].astype(BF)
        vsum = vsum + x * x
        rsum = rsum + res * res
    return vsum, rsum


def finished_planes(terms, cells, z0, carry, links, outs, out, low, high, ends, step):
    ready = []
    for z in ends:
        carry = one_plane(terms, cells, z, z0, carry, links.get(z), outs(z))
        ready.append((z, z + 1))
    for first, end in cuts(low, high, step):
        carry = lax.fori_loop(
            first, end, lambda z, c: one_plane(terms, cells, z, z0, c, None, outs(first)), carry
        )
        for cut in ready:
            out.send(*cut)
        ready = [(first, end)]
    return carry, ready


def part_one_kernel(chunks, parts, planes, split, me_ref, *rest):
    nz = parts * len(chunks)
    z_refs, rest = rest[:nz], rest[nz:]
    link_ref, eig_ref, stiff_ref, damp_ref, mass_ref = rest[:5]
    vec_ref, res_ref, edge_ref, sum_ref, cells, vec_buf, res_buf, sem = rest[5:]
    vecs = vec_ref.shape[0]
    tiles = WID * WID // LANES
    for i, chunk in enumerate(chunks):
        unpack(cells, 0, chunk, me_ref[0], parts, z_refs[i * parts : (i + 1) * parts], vecs - 8)
    terms = Terms(eig_ref, stiff_ref, damp_ref, mass_ref)
    moved = (planes - 1 - split) * WID * WID
    outs = lambda z: (vec_buf, res_buf, moved if z == planes - 1 else 0)
    out = Output((vec_ref, res_ref), (vec_buf, res_buf), sem, {planes - 1: planes - 1 - split})
    zero = jnp.zeros((NP, LANES), F32)
    links = {0: (link_ref, 0, 1), planes - 1: (link_ref, tiles, -1)}
    carry, ready = finished_planes(
        terms, cells, 0, (zero, zero), links, outs, out, 1, split, (0, planes - 1), 1
    )
    edge_ref[0 : 2 * tiles] = cells[(split - 1) * tiles : (split + 1) * tiles]
    edge_ref[2 * tiles : 4 * tiles] = cells[(planes - 2) * tiles : planes * tiles]
    sum_ref[0], sum_ref[1] = carry
    for cut in ready:
        out.send(*cut)
    out.wait()


def part_two_kernel(chunk, parts, planes, split, me_ref, *rest):
    z_refs, rest = rest[:parts], rest[parts:]
    edge_ref, eig_ref, stiff_ref, damp_ref, mass_ref, early_ref, _, _ = rest[:8]
    vec_ref, res_ref, out_ref, cells, vec_buf, res_buf, sem = rest[8:]
    vecs = vec_ref.shape[0]
    tiles = WID * WID // LANES
    z0 = split - 1
    cells[0 : 2 * tiles] = edge_ref[0 : 2 * tiles]
    cells[(planes - 2 - z0) * tiles : (planes - z0) * tiles] = edge_ref[2 * tiles : 4 * tiles]
    unpack(cells, z0 * tiles, chunk, me_ref[0], parts, z_refs, vecs - 8)
    terms = Terms(eig_ref, stiff_ref, damp_ref, mass_ref)
    outs = lambda z: (vec_buf, res_buf, split * WID * WID)
    out = Output((vec_ref, res_ref), (vec_buf, res_buf), sem, {None: split})
    carry = (early_ref[0], early_ref[1])
    carry, ready = finished_planes(terms, cells, z0, carry, {}, outs, out, split, planes - 1, (), 1)
    vsum, rsum = carry
    vrow = jnp.broadcast_to(jnp.sum(vsum, axis=1, keepdims=True), (NP, LANES))
    rrow = jnp.broadcast_to(jnp.sum(rsum, axis=1, keepdims=True), (NP, LANES))
    sub = lax.broadcasted_iota(jnp.int32, (NP, LANES), 0)
    wide = lax.broadcasted_iota(jnp.int32, (NP, LANES), 1)
    both = jnp.where((sub == wide) & (sub < vecs), vrow, 0.0)
    both = both + jnp.where((sub + NP == wide) & (sub < vecs), rrow, 0.0)
    line = jnp.sum(both, axis=0, keepdims=True)
    out_ref[...] = jnp.broadcast_to(line[None], out_ref.shape)
    for cut in ready:
        out.send(*cut)
    out.wait()


def buffers(planes, kept_planes, vecs):
    tiles = WID * WID // LANES
    return [
        pltpu.VMEM((planes * tiles, NP, LANES), F32),
        pltpu.VMEM((vecs, kept_planes * WID * WID), BF),
        pltpu.VMEM((vecs, kept_planes * WID * WID), BF),
        pltpu.SemaphoreType.DMA((24,)),
    ]


def part_one(me, chunks, zs, link, eig, diagonals, vecs, rows_local, parts, split):
    planes = rows_local // (WID * WID)
    tiles = WID * WID // LANES
    whole = jax.ShapeDtypeStruct((vecs, rows_local), BF)
    return pl.pallas_call(
        functools.partial(part_one_kernel, chunks, parts, planes, split),
        out_shape=(
            whole,
            whole,
            jax.ShapeDtypeStruct((4 * tiles, NP, LANES), F32),
            jax.ShapeDtypeStruct((2, NP, LANES), F32),
        ),
        in_specs=[SMEM] + [VMEM] * (len(zs) + 5),
        out_specs=(ANY, ANY, VMEM, VMEM),
        scratch_shapes=buffers(planes, split + 1, vecs),
        compiler_params=params(20),
        cost_estimate=cost(2000 * NP * rows_local, 4 * NP * rows_local),
        name="part_one",
    )(me, *zs, link, eig, *diagonals)


def part_two(me, chunk, zs, edge, eig, diagonals, early, vec, res, parts, split, copies):
    vecs, rows_local = vec.shape
    planes = rows_local // (WID * WID)
    whole = jax.ShapeDtypeStruct((vecs, rows_local), BF)
    first = 1 + parts + 6
    return pl.pallas_call(
        functools.partial(part_two_kernel, chunk, parts, planes, split),
        out_shape=(whole, whole, jax.ShapeDtypeStruct((copies, 1, LANES), F32)),
        in_specs=[SMEM] + [VMEM] * (parts + 6) + [ANY, ANY],
        out_specs=(ANY, ANY, VMEM),
        scratch_shapes=buffers(planes - split + 1, planes - 1 - split, vecs),
        input_output_aliases={first: 0, first + 1: 1},
        compiler_params=params(20),
        cost_estimate=cost(2000 * NP * rows_local, 4 * NP * rows_local),
        name="part_two",
    )(me, *zs, edge, eig, *diagonals, early, vec, res)


def kept(value):
    def kernel(from_ref, to_ref):
        to_ref[...] = from_ref[...]

    return pl.pallas_call(
        kernel,
        out_shape=jax.ShapeDtypeStruct(value.shape, value.dtype),
        in_specs=[VMEM],
        out_specs=VMEM,
        compiler_params=params(4),
        cost_estimate=cost(1, 4 * value.size),
        name="kept",
    )(value)


def exchanged(arrays, axis):
    return [arrays[0]] + [from_behind(arrays[k], axis, k) for k in range(1, len(arrays))]


def on_device(
    basis,
    coefficients,
    eigen_values,
    stiffness,
    damping,
    mass,
    link_count,
    lower_cells,
    upper_cells,
):
    parts = lax.axis_size("vecs")
    subdomains = lax.axis_size("rows")
    vecs = eigen_values.shape[0]
    ranks, rows_local = basis.shape
    planes = rows_local // (WID * WID)
    me = lax.axis_index("vecs").astype(jnp.int32)[None]
    ends = Chunk(None, 4, parts, planes)
    middle = (planes - 4) // 2 + 4
    one = Chunk(2, middle - 2, parts, planes)
    two = Chunk(middle, planes - 2 - middle, parts, planes)
    wide_count = jnp.broadcast_to(link_count[:, None], (1, LANES))
    lists = jnp.concatenate([lower_cells, upper_cells, wide_count], axis=1)
    (ends_out,) = pack(me, basis, [ends], parts)
    ends_out = exchanged(ends_out, "vecs")
    one_out, two_out = pack(me, basis, [one, two], parts)
    one_out = exchanged(one_out, "vecs")
    down = from_behind(lists, "rows", 1)
    matrix = spread_coefficients(me, coefficients, parts, ranks, vecs)
    z_ends = mix(matrix, ends_out, 0, ends.seg, vecs)
    z_ends = exchanged(z_ends, "vecs")
    two_out = exchanged(two_out, "vecs")
    hots = one_hots(min(ends.seg, 256), down, lower_cells, upper_cells, wide_count[:, :1])
    one_out[0], two_out[0] = kept(one_out[0]), kept(two_out[0])
    z_one = mix(matrix, one_out, 0, one.seg, vecs)
    z_one = exchanged(z_one, "vecs")
    plane_low, plane_high = end_planes(me, z_ends)
    from_below = from_behind(plane_high, "rows", 1)
    from_above = from_behind(plane_low, "rows", -1)
    link = link_terms(from_below, from_above, hots)
    z_two = mix(matrix, two_out, 0, two.seg, vecs)
    z_two = exchanged(z_two, "vecs")
    diagonals = [a.reshape(rows_local // LANES, LANES) for a in (stiffness, damping, mass)]
    eig = eigen_values[None, :]
    split = middle - 1
    eigvecs, residuals, edge, sums = part_one(
        me, [ends, one], z_ends + z_one, link, eig, diagonals, vecs, rows_local, parts,
        split,
    )
    eigvecs, residuals, sums = part_two(
        me, two, z_two, edge, eig, diagonals, sums, eigvecs, residuals, parts, split,
        subdomains,
    )
    total = lax.all_to_all(sums, "rows", 0, 0, tiled=True).sum(axis=(0, 1))
    vector_sq, residual_sq = total[:vecs], total[NP : NP + vecs]
    relative_norms = jnp.sqrt(residual_sq) / jnp.sqrt(vector_sq + 1.0)
    return (eigvecs, residuals, relative_norms)


def solution(mesh):
    placed = (
        P("vecs", "rows"),
        P(),
        P("vecs"),
        P("rows"),
        P("rows"),
        P("rows"),
        P("rows"),
        P("rows", None),
        P("rows", None),
    )
    return jax.shard_map(
        on_device,
        mesh=mesh,
        in_specs=placed,
        out_specs=(P("vecs", "rows"), P("vecs", "rows"), P("vecs")),
        check_vma=False,
    )
```
